128 devices in a mesh: row: 16 (over z, x), col: 8 (over y, core).
Axes of the slice: x: 4, y: 4, z: 4, core: 2. Of those that a mesh axis runs over, the one named last changes fastest.
Arguments:
- density_first: bfloat16 [12288, 12288], P('row', 'col'), may hold values from -0.0068359375 to 0.0068359375
- density_second: bfloat16 [12288, 12288], P('row', 'col'), may hold values from -0.0068359375 to 0.0068359375
- basis: bfloat16 [256, 4096, 896], P(('row', 'col')), may hold values from -6 to 6
- tile_list: int32 [256, 7], P(('row', 'col')), may hold values from 0 to 95, as said below
- tile_count: int32 [256], P(('row', 'col')), may hold values from 5 to 7, as said below
- point_count: int32 [256], P(('row', 'col')), may hold values from 1024 to 4096, as said below
- offsets: float32 [3, 256, 4096], P(None, ('row', 'col')), may hold values from -5 to 5
- weights: float32 [256, 4096], P(('row', 'col')), may hold values from 0.05 to 1
- atom_of_point: int32 [256, 4096], P(('row', 'col')), may hold values from 0 to 1023, as said below
Outputs:
- density: float32 [2, 256, 4096], P(None, ('row', 'col'))
- moments: float32 [2, 9, 1024], replicated
The draws below stay inside these ranges and needn't reach their ends.
Inputs may be any that keep to these rules, and one draw needn't show every extreme that they name: `tile_list`: the 7 tile numbers of each batch are 7 consecutive numbers in some order. `tile_count`: some batch has 7. `point_count`: some batch has 4096. `atom_of_point`: the points of batch g belong to atoms (g * 4 + j) mod 1024 with j from 0 to 7.
All inputs are finite; a program needn't handle non-finite values.
Results may differ from the reference program's by a relative error of at most 0.0003.
Values may be sent and summed in bfloat16 or wider, within the bound.
A program may use at most 192 MiB of HBM per device.

```python
import math
import jax
import jax.numpy as jnp
from jax import lax

TILE = 128
NB = 12288
KT = 7
PTS = 4096
ATOMS = 1024
NT = 96
BATCHES = 256
N_ROW = 16
N_COL = 8


def lift_one(key, values, top):
    chosen = jax.random.randint(jax.random.fold_in(key, 17), (), 0, values.shape[0])
    return jnp.where(jnp.arange(values.shape[0]) == chosen, top, values).astype(jnp.int32)


def draw_tile_list(key, part):
    start_key = jax.random.fold_in(key, 3)
    order_key = jax.random.fold_in(key, 5)
    starts = jax.random.randint(start_key, (BATCHES, 1), 0, NT - KT + 1)
    order_keys = jax.random.split(order_key, BATCHES)
    orders = jax.vmap(lambda single: jax.random.permutation(single, KT))(order_keys)
    return (starts + orders).astype(jnp.int32)


def draw_tile_count(key, part):
    base = jax.random.randint(jax.random.fold_in(key, 7), (BATCHES,), KT - 2, KT + 1)
    return lift_one(key, base, KT)


def draw_point_count(key, part):
    base = jax.random.randint(jax.random.fold_in(key, 11), (BATCHES,), PTS // 4, PTS + 1)
    return lift_one(key, base, PTS)


def draw_atom_of_point(key, part):
    base = (jnp.arange(BATCHES, dtype=jnp.int32) * ATOMS // BATCHES)[:, None]
    spread = jax.random.randint(jax.random.fold_in(key, 13), (BATCHES, PTS), 0, 8)
    return ((base + spread) % ATOMS).astype(jnp.int32)


def level_of(own_key, extent, pieces, low, largest):
    def one(dim, blocks):
        steps = jax.random.uniform(jax.random.fold_in(jax.random.fold_in(own_key, 6), dim), (blocks,), jnp.float32, low / len(pieces), largest / len(pieces))
        return jnp.repeat(jnp.exp(steps), extent[dim] // blocks).reshape((-1,) + (1,) * (len(extent) - dim - 1))

    gain = one(*pieces[0])
    for cut in pieces[1:]:
        gain = gain * one(*cut)
    return gain


def normal_values(key, dims, scale, reach, pieces=(), kind=jnp.bfloat16):
    entries = jax.random.normal(key, dims, jnp.float32) * scale
    if len(pieces) > 0:
        entries = level_of(key, dims, pieces, -0.22, 0.18) * entries
    return jnp.clip(entries, min=-reach, max=reach).astype(kind)


def setup_inputs(seed: int = 0) -> dict:
    seeds = jax.random.split(jax.random.key(seed), 10)
    density_first = normal_values(seeds[0], (NB, NB), ((KT * TILE) ** 2) ** -0.5, 0.0068359375, ((0, 16), (1, 8)))
    density_second = normal_values(seeds[1], (NB, NB), ((KT * TILE) ** 2) ** -0.5, 0.0068359375, ((0, 16), (1, 8)))
    basis = normal_values(seeds[2], (BATCHES, PTS, KT * TILE), 1.0, 6.0, ((0, 128),))
    tile_list = draw_tile_list(jax.random.fold_in(seeds[9], 71), 0)
    tile_count = draw_tile_count(jax.random.fold_in(seeds[9], 71), 0)
    point_count = draw_point_count(jax.random.fold_in(seeds[9], 71), 0)
    offsets = normal_values(seeds[6], (3, BATCHES, PTS), 1.0, 5.0, ((1, 128),), jnp.float32)
    weights = jnp.clip(jnp.exp(math.log(1.0) - 2.9957323 * jax.random.uniform(seeds[7], (BATCHES, PTS), jnp.float32) ** level_of(seeds[7], (BATCHES, PTS), ((0, 128),), -0.2, 0.2)), 0.05, 1.0)
    atom_of_point = draw_atom_of_point(jax.random.fold_in(seeds[9], 71), 0)
    return dict(density_first=density_first, density_second=density_second, basis=basis, tile_list=tile_list, tile_count=tile_count, point_count=point_count, offsets=offsets, weights=weights, atom_of_point=atom_of_point)


def harmonics(offsets):
    first_axis = offsets[0]
    second_axis = offsets[1]
    third_axis = offsets[2]
    radius_sq = first_axis * first_axis + second_axis * second_axis + third_axis * third_axis
    return jnp.stack([jnp.ones_like(first_axis), first_axis, second_axis, third_axis,
                      first_axis * second_axis, second_axis * third_axis,
                      3.0 * third_axis * third_axis - radius_sq,
                      first_axis * third_axis,
                      first_axis * first_axis - second_axis * second_axis])


def storage_index(tiles, parts):
    per_part = NT // parts
    return ((tiles % parts) * per_part + tiles // parts).astype(jnp.int32)


def batch_density(stored_first, stored_second, values, tiles, live_tiles, live_points):
    inside = jnp.arange(TILE, dtype=jnp.int32)[None, :]
    rows = (storage_index(tiles, N_ROW)[:, None] * TILE + inside).reshape(-1)
    cols = (storage_index(tiles, N_COL)[:, None] * TILE + inside).reshape(-1)
    col_mask = jnp.repeat((jnp.arange(KT) < live_tiles).astype(jnp.bfloat16), TILE)
    masked = values * col_mask[None, :]
    point_mask = (jnp.arange(PTS) < live_points).astype(jnp.float32)
    results = []
    for stored in (stored_first, stored_second):
        block = stored[rows[:, None], cols[None, :]]
        product = jnp.dot(masked, block, preferred_element_type=jnp.float32)
        results.append(jnp.sum(product * masked.astype(jnp.float32), axis=1) * point_mask)
    return jnp.stack(results)


def reference(density_first, density_second, basis, tile_list, tile_count, point_count, offsets, weights, atom_of_point):
    def per_batch(inputs):
        values, tiles, live_tiles, live_points = inputs
        return batch_density(density_first, density_second, values, tiles, live_tiles, live_points)

    stacked = lax.map(per_batch, (basis, tile_list, tile_count, point_count))
    density = jnp.transpose(stacked, (1, 0, 2))
    harmonic = harmonics(offsets)
    moment_terms = density[:, None] * (weights[None, None] * harmonic[None])
    flat_terms = moment_terms.reshape(2 * 9, -1).T
    summed = jax.ops.segment_sum(flat_terms, atom_of_point.reshape(-1), num_segments=ATOMS)
    moments = summed.T.reshape(2, 9, ATOMS)
    return density, moments
```

```python
import functools

import jax
import jax.numpy as jnp
from jax import lax
from jax.experimental import pallas as pl
from jax.experimental.pallas import tpu as pltpu
from jax.sharding import Mesh
from jax.sharding import PartitionSpec as P

TILE = 128
ATOMS = 1024
ROW = ("row_0", "row_1")
COL = ("col_0", "col_1")
ROW_COL = ("row_0", "row_1", "col_0", "col_1")
KT = 7
N_ROW = 16
N_COL = 8
DEVS = N_ROW * N_COL
NT = 96
STARTS = NT - KT + 1
LOCAL_T = NT // N_ROW
LOCAL_U = NT // N_COL
BLOCK = 512
GROUPS = BLOCK // TILE
F32 = jnp.float32
BF16 = jnp.bfloat16
I16 = jnp.int16
I32 = jnp.int32
VMEM_LIMIT = 60 * 1024 * 1024
SMEM_SPEC = pl.BlockSpec(memory_space=pltpu.SMEM)
VMEM_SPEC = pl.BlockSpec(memory_space=pltpu.VMEM)
ANY_SPEC = pl.BlockSpec(memory_space=pl.ANY)


def extract_kernel(meta, first, second, out, tiles, sems):
    r = meta[0]
    c = meta[1]
    e = lax.bitwise_and(c - r, 7)

    def fetch(m, ul, t):
        column = r + 16 * t + e - 8 * ul - c
        column = jnp.clip(lax.shift_right_arithmetic(column, 3), 0, LOCAL_U - 1)
        source = (first, second)[m]
        return pltpu.make_async_copy(
            source.at[pl.ds(t * TILE, TILE), pl.ds(pl.multiple_of(column * TILE, TILE), TILE)],
            tiles.at[m, ul, t],
            sems.at[m, ul, t],
        )

    todo = [(m, ul, t) for m in range(2) for ul in range(2) for t in range(LOCAL_T)]
    for item in todo:
        fetch(*item).start()
    out[...] = jnp.zeros(out.shape, out.dtype)
    for m, ul, t in todo:
        fetch(m, ul, t).wait()
        row_tile = r + 16 * t
        d = e if ul == 0 else 8 - e
        near = d <= 3
        if ul == 0:
            key = jnp.where(near, row_tile, row_tile + d)
            turned = (e >= 1) & (e <= 3)
        else:
            key = jnp.where(near, row_tile - d, row_tile)
            turned = e <= 4
        kind = jnp.where(near, d, 7 - d)
        q = lax.bitwise_and(kind + 4 * m + lax.shift_right_arithmetic(key, 4), 7)
        tile = tiles[m, ul, t].astype(F32)
        tile = jnp.where(turned, tile.T, tile)
        out[:, q, m, ul] = tile.reshape(N_ROW, 8, TILE).astype(BF16)


def extract(meta, first, second):
    return pl.pallas_call(
        extract_kernel,
        name="extract",
        out_shape=jax.ShapeDtypeStruct((N_ROW, N_COL, 2, 2, 8, TILE), BF16),
        in_specs=[SMEM_SPEC, ANY_SPEC, ANY_SPEC],
        out_specs=VMEM_SPEC,
        scratch_shapes=[
            pltpu.VMEM((2, 2, LOCAL_T, TILE, TILE), BF16),
            pltpu.SemaphoreType.DMA((2, 2, LOCAL_T)),
        ],
        compiler_params=pltpu.CompilerParams(vmem_limit_bytes=VMEM_LIMIT),
    )(meta, first, second)


def encode(value):
    size = jnp.abs(value)
    safe = jnp.maximum(size, 2.0**-38)
    power = jnp.floor(jnp.log2(safe))
    code = (power + 37.0) * 1024.0 + safe * jnp.exp2(10.0 - power)
    code = jnp.clip(jnp.floor(code + 0.5), 0.0, 32767.0)
    code = jnp.where(size >= 2.0**-38, code, 0.0)
    code = jnp.where(value < 0.0, -code, code)
    return code.astype(I32).astype(I16)


def decode(code):
    code = code.astype(I32)
    size = jnp.abs(code)
    power = lax.shift_right_logical(size, 10).astype(F32)
    fraction = (lax.bitwise_and(size, 1023) + 1024).astype(F32)
    value = fraction * jnp.exp2(power - 48.0)
    value = jnp.where(size > 0, value, 0.0)
    return jnp.where(code < 0, -value, value)


def pack_kernel(meta, starts, slices, out, table, windows, sem):
    q = meta[1]

    def kind_of(k):
        return lax.bitwise_and(q - lax.shift_right_arithmetic(k, 4), 7)

    def fill(k, carry):
        which = kind_of(k)
        kind = lax.bitwise_and(which, 3)
        m = lax.shift_right_arithmetic(which, 2)

        def owner(row_tile, col_tile):
            return lax.bitwise_and(row_tile, 15) * 8 + lax.bitwise_and(col_tile, 7)

        far = k + kind
        upper = slices[owner(k, far), m, 0].astype(F32)
        lower = slices[owner(far, k), m, 1].astype(F32)
        table[2 * k] = encode(jnp.where(kind > 0, upper + lower, upper))
        near = k - 7 + kind
        upper = slices[owner(near, k), m, 0].astype(F32)
        lower = slices[owner(k, near), m, 1].astype(F32)
        table[2 * k + 1] = encode(upper + lower)
        return carry

    lax.fori_loop(0, NT, fill, 0, unroll=4)

    def window(a, carry):
        for t in range(KT):
            kind = lax.bitwise_and(kind_of(a + t), 3)
            wraps = (kind > 0) & (t + kind > KT - 1)
            windows[a, t] = table[2 * (a + t) + wraps.astype(I32)]
        return carry

    lax.fori_loop(0, STARTS, window, 0, unroll=2)

    def send(d, carry):
        for b in range(2):
            pltpu.make_async_copy(windows.at[starts[2 * d + b]], out.at[b, d], sem).start()
        return carry

    lax.fori_loop(0, DEVS, send, 0, unroll=4)
    pltpu.make_async_copy(out, out, sem).wait()


def pack(meta, starts, slices):
    return pl.pallas_call(
        pack_kernel,
        name="pack",
        out_shape=jax.ShapeDtypeStruct((2, DEVS, KT, 8, TILE), I16),
        in_specs=[SMEM_SPEC, SMEM_SPEC, VMEM_SPEC],
        out_specs=ANY_SPEC,
        scratch_shapes=[
            pltpu.VMEM((2 * NT, 8, TILE), I16),
            pltpu.VMEM((STARTS, KT, 8, TILE), I16),
            pltpu.SemaphoreType.DMA,
        ],
        compiler_params=pltpu.CompilerParams(vmem_limit_bytes=VMEM_LIMIT),
    )(meta, starts, slices)


def harmonics(x, y, z):
    radius_sq = x * x + y * y + z * z
    return [
        None,
        x,
        y,
        z,
        x * y,
        y * z,
        3.0 * z * z - radius_sq,
        x * z,
        x * x - y * y,
    ]


def batch_kernel(
    batch, info, arrived, basis, offsets, weights, atoms, dens, moments, matrix, phi, sums, sems
):
    start = info[0]
    count = info[1]
    base = info[2]
    blocks = lax.div(count + (BLOCK - 1), BLOCK)

    def fetch(block, slot, j):
        place = pl.multiple_of(info[3 + j % KT] * TILE, TILE)
        return pltpu.make_async_copy(
            basis.at[batch, pl.ds(pl.multiple_of(block * BLOCK, BLOCK), BLOCK), pl.ds(place, TILE)],
            phi.at[slot, :, pl.ds(j * TILE, TILE)],
            sems.at[slot, j],
        )

    for j in range(KT + 3):
        fetch(0, 0, j).start()

    for t in range(KT):
        turn = lax.shift_right_arithmetic(start + t, 4)
        for kind in range(4):
            live = (info[10 + t] * info[10 + (t + kind) % KT]).astype(F32)
            for m in range(2):
                q = lax.bitwise_and(kind + 4 * m + turn, 7)
                value = decode(arrived[:, q, t]).reshape(TILE, TILE) * live
                high = value.astype(BF16)
                low = (value - high.astype(F32)).astype(BF16)
                columns = pl.ds(m * TILE, TILE)
                matrix[t, pl.ds(kind * TILE, TILE), columns] = high
                matrix[t, pl.ds((4 + kind) * TILE, TILE), columns] = low

    dens[...] = jnp.zeros(dens.shape, F32)

    def step(block, carry):
        slot = lax.bitwise_and(block, 1)

        @pl.when(block + 1 < blocks)
        def _():
            for j in range(KT + 3):
                fetch(block + 1, 1 - slot, j).start()

        for j in range(KT + 3):
            fetch(block, slot, j).wait()
        total = jnp.zeros((BLOCK, 2 * TILE), F32)
        for t in range(KT):
            left = phi[slot, :, pl.ds(t * TILE, 4 * TILE)]
            product = jnp.dot(
                left, matrix[t, pl.ds(0, 4 * TILE), :], preferred_element_type=F32
            ) + jnp.dot(left, matrix[t, pl.ds(4 * TILE, 4 * TILE), :], preferred_element_type=F32)
            own = left[:, :TILE].astype(F32)
            total = total + product * jnp.concatenate([own, own], axis=1)
        for m in range(2):
            for i in range(GROUPS):
                part = total[i * TILE : (i + 1) * TILE, m * TILE : (m + 1) * TILE]
                dens[m, pl.ds(block * GROUPS + i, 1), :] = jnp.sum(part.T, axis=0, keepdims=True)
        return carry

    lax.fori_loop(0, blocks, step, 0)

    rows = dens.shape[1]
    place = lax.broadcasted_iota(I32, (rows, TILE), 0) * TILE + lax.broadcasted_iota(
        I32, (rows, TILE), 1
    )
    inside = place < count
    harmonic = harmonics(offsets[0], offsets[1], offsets[2])
    weight = weights[...]
    factors = [weight] + [weight * item for item in harmonic[1:]]
    hits = [atoms[...] == lax.bitwise_and(base + j, ATOMS - 1) for j in range(8)]
    sums[...] = jnp.zeros(sums.shape, F32)
    for m in range(2):
        value = jnp.where(inside, dens[m], 0.0)
        dens[m] = value
        for h in range(9):
            term = value * factors[h]
            for j in range(8):
                picked = jnp.where(hits[j], term, 0.0)
                sums[pl.ds(j * 18 + m * 9 + h, 1), :] = jnp.sum(picked, axis=0, keepdims=True)
    for i in range(2):
        part = sums[pl.ds(i * TILE, TILE), :]
        moments[pl.ds(i, 1), :] = jnp.sum(part.T, axis=0, keepdims=True)


def batch_density(batch, info, arrived, basis, offsets, weights, atoms):
    points = basis.shape[1]
    rows = points // TILE
    return pl.pallas_call(
        functools.partial(batch_kernel, batch),
        name="batch_density",
        out_shape=(
            jax.ShapeDtypeStruct((2, rows, TILE), F32),
            jax.ShapeDtypeStruct((2, TILE), F32),
        ),
        in_specs=[SMEM_SPEC, VMEM_SPEC, ANY_SPEC, VMEM_SPEC, VMEM_SPEC, VMEM_SPEC],
        out_specs=(VMEM_SPEC, VMEM_SPEC),
        scratch_shapes=[
            pltpu.VMEM((KT, 8 * TILE, 2 * TILE), BF16),
            pltpu.VMEM((2, BLOCK, (KT + 3) * TILE), BF16),
            pltpu.VMEM((2 * TILE, TILE), F32),
            pltpu.SemaphoreType.DMA((2, KT + 3)),
        ],
        compiler_params=pltpu.CompilerParams(vmem_limit_bytes=VMEM_LIMIT),
        cost_estimate=pl.CostEstimate(
            flops=2 * points * 1024 * 256 * KT, bytes_accessed=12_000_000, transcendentals=0
        ),
    )(info, arrived, basis, offsets, weights, atoms)


def exchange(value):
    return lax.all_to_all(value, ROW_COL, split_axis=0, concat_axis=0, tiled=True)


def local(
    density_first,
    density_second,
    basis,
    tile_list,
    tile_count,
    point_count,
    offsets,
    weights,
    atom_of_point,
):
    points = basis.shape[1]
    rows = points // TILE
    my_row = lax.axis_index(ROW).astype(I32)
    my_col = lax.axis_index(COL).astype(I32)
    device = my_row * N_COL + my_col
    meta = jnp.stack([my_row, my_col])
    own_start = jnp.min(tile_list, axis=1)
    starts = exchange(jnp.broadcast_to(own_start[None], (DEVS, 2))).reshape(-1)

    slices = extract(meta, density_first, density_second)
    slices = exchange(slices.reshape(DEVS, 2, 2, 8, TILE))
    outgoing = pack(meta, starts, slices)
    arrived = [exchange(outgoing[b]) for b in range(2)]

    place = jnp.argsort(tile_list, axis=1).astype(I32)
    live = (place < tile_count[:, None]).astype(I32)
    base = (2 * device + jnp.arange(2, dtype=I32)) * 4 % ATOMS
    info = jnp.concatenate(
        [own_start[:, None], point_count[:, None], base[:, None], place, live], axis=1
    )
    dens = []
    moments = []
    for b in range(2):
        one, part = batch_density(
            b,
            info[b],
            arrived[b].reshape(N_ROW, N_COL, KT, 8, TILE),
            basis,
            offsets[:, b].reshape(3, rows, TILE),
            weights[b].reshape(rows, TILE),
            atom_of_point[b].reshape(rows, TILE),
        )
        dens.append(one.reshape(2, points))
        moments.append(part.reshape(-1)[: 8 * 18])
    density = jnp.stack(dens, axis=1)
    half = 4 * 18
    own = jnp.concatenate(
        [moments[0][:half], moments[0][half:] + moments[1][:half], moments[1][half:]]
    )
    spare = jnp.zeros((2 * TILE - 3 * half,), F32)
    own = jnp.concatenate([own, spare])
    everyone = exchange(jnp.broadcast_to(own[None], (DEVS, 2 * TILE)))
    main = everyone[:, : 2 * half]
    extra = jnp.roll(everyone[:, 2 * half : 3 * half], 1, axis=0)
    whole = main + jnp.concatenate([extra, jnp.zeros_like(extra)], axis=1)
    whole = whole.reshape(ATOMS, 18).T.reshape(2, 9, ATOMS)
    return (density, whole)


def solution(mesh):
    torus = Mesh(mesh.devices.reshape(4, 4, 4, 2), ("row_0", "row_1", "col_0", "col_1"))
    in_specs = (
        P(ROW, COL),
        P(ROW, COL),
        P(ROW_COL, None, None),
        P(ROW_COL, None),
        P(ROW_COL),
        P(ROW_COL),
        P(None, ROW_COL, None),
        P(ROW_COL, None),
        P(ROW_COL, None),
    )
    out_specs = (P(None, ROW_COL, None), P())
    return jax.shard_map(local, mesh=torus, in_specs=in_specs, out_specs=out_specs, check_vma=False)
```

```python
import functools

import jax
import jax.numpy as jnp
from jax import lax
from jax.experimental import pallas as pl
from jax.experimental.pallas import tpu as pltpu
from jax.sharding import Mesh
from jax.sharding import PartitionSpec as P

TILE = 128
ATOMS = 1024
ROW = ("row_0", "row_1")
COL = ("col_0", "col_1")
ROW_COL = ("row_0", "row_1", "col_0", "col_1")
KT = 7
N_ROW = 16
N_COL = 8
DEVS = N_ROW * N_COL
NT = 96
STARTS = NT - KT + 1
LOCAL_T = NT // N_ROW
LOCAL_U = NT // N_COL
BLOCK = 512
GROUPS = BLOCK // TILE
F32 = jnp.float32
BF16 = jnp.bfloat16
I16 = jnp.int16
I32 = jnp.int32
VMEM_LIMIT = 60 * 1024 * 1024
SMEM_SPEC = pl.BlockSpec(memory_space=pltpu.SMEM)
VMEM_SPEC = pl.BlockSpec(memory_space=pltpu.VMEM)
ANY_SPEC = pl.BlockSpec(memory_space=pl.ANY)


def extract_kernel(meta, first, second, out, tiles, sems):
    r = meta[0]
    c = meta[1]
    e = lax.bitwise_and(c - r, 7)

    def fetch(m, ul, t):
        column = r + 16 * t + e - 8 * ul - c
        column = jnp.clip(lax.shift_right_arithmetic(column, 3), 0, LOCAL_U - 1)
        source = (first, second)[m]
        return pltpu.make_async_copy(
            source.at[pl.ds(t * TILE, TILE), pl.ds(pl.multiple_of(column * TILE, TILE), TILE)],
            tiles.at[m, ul, t],
            sems.at[m, ul, t],
        )

    todo = [(m, ul, t) for m in range(2) for ul in range(2) for t in range(LOCAL_T)]
    for item in todo:
        fetch(*item).start()
    out[...] = jnp.zeros(out.shape, out.dtype)
    for m, ul, t in todo:
        fetch(m, ul, t).wait()
        row_tile = r + 16 * t
        d = e if ul == 0 else 8 - e
        near = d <= 3
        if ul == 0:
            key = jnp.where(near, row_tile, row_tile + d)
            turned = (e >= 1) & (e <= 3)
        else:
            key = jnp.where(near, row_tile - d, row_tile)
            turned = e <= 4
        kind = jnp.where(near, d, 7 - d)
        q = lax.bitwise_and(kind + 4 * m + lax.shift_right_arithmetic(key, 4), 7)
        tile = tiles[m, ul, t].astype(F32)
        tile = jnp.where(turned, tile.T, tile)
        out[:, q, m, ul] = tile.reshape(N_ROW, 8, TILE).astype(BF16)


def extract(meta, first, second):
    return pl.pallas_call(
        extract_kernel,
        name="extract",
        out_shape=jax.ShapeDtypeStruct((N_ROW, N_COL, 2, 2, 8, TILE), BF16),
        in_specs=[SMEM_SPEC, ANY_SPEC, ANY_SPEC],
        out_specs=VMEM_SPEC,
        scratch_shapes=[
            pltpu.VMEM((2, 2, LOCAL_T, TILE, TILE), BF16),
            pltpu.SemaphoreType.DMA((2, 2, LOCAL_T)),
        ],
        compiler_params=pltpu.CompilerParams(vmem_limit_bytes=VMEM_LIMIT),
    )(meta, first, second)


def encode(value):
    size = jnp.abs(value)
    safe = jnp.maximum(size, 2.0**-38)
    power = jnp.floor(jnp.log2(safe))
    code = (power + 37.0) * 1024.0 + safe * jnp.exp2(10.0 - power)
    code = jnp.clip(jnp.floor(code + 0.5), 0.0, 32767.0)
    code = jnp.where(size >= 2.0**-38, code, 0.0)
    code = jnp.where(value < 0.0, -code, code)
    return code.astype(I32).astype(I16)


def decode(code):
    code = code.astype(I32)
    size = jnp.abs(code)
    power = lax.shift_right_logical(size, 10).astype(F32)
    fraction = (lax.bitwise_and(size, 1023) + 1024).astype(F32)
    value = fraction * jnp.exp2(power - 48.0)
    value = jnp.where(size > 0, value, 0.0)
    return jnp.where(code < 0, -value, value)


MESH_ID = pl.DeviceIdType.MESH


def position():
    return [lax.axis_index(name) for name in ROW_COL]


def flat(spot):
    return ((spot[0] * 4 + spot[1]) * 4 + spot[2]) * 2 + spot[3]


def partner(spot, i):
    j = (i * 37) % DEVS
    away = [j // 32, (j // 8) % 4, (j // 2) % 4, j % 2]
    return [(p + o) % n for p, o, n in zip(spot, away, (4, 4, 4, 2), strict=True)]


def wait_all(ref, sem):
    pltpu.make_async_copy(ref, ref, sem).wait()


def spread_kernel(slices, own, out, starts, send_sems, recv_sems, here_sems):
    spot = position()
    me = flat(spot)
    mine = pltpu.make_async_copy(own, starts.at[me], here_sems.at[0])
    mine.start()
    kept = pltpu.make_async_copy(slices.at[me], out.at[me], here_sems.at[1])
    kept.start()

    def send_start(i, carry):
        pltpu.make_async_remote_copy(
            src_ref=own,
            dst_ref=starts.at[me],
            send_sem=send_sems.at[0],
            recv_sem=recv_sems.at[0],
            device_id=tuple(partner(spot, i)),
            device_id_type=MESH_ID,
        ).start()
        return carry

    def send_slices(i, carry):
        to = partner(spot, i)
        pltpu.make_async_remote_copy(
            src_ref=slices.at[flat(to)],
            dst_ref=out.at[me],
            send_sem=send_sems.at[1],
            recv_sem=recv_sems.at[1],
            device_id=tuple(to),
            device_id_type=MESH_ID,
        ).start()
        return carry

    lax.fori_loop(1, DEVS, send_start, 0)
    lax.fori_loop(1, DEVS, send_slices, 0)
    mine.wait()
    kept.wait()
    others = pl.ds(0, DEVS - 1)
    wait_all(starts.at[others], send_sems.at[0])
    wait_all(starts.at[others], recv_sems.at[0])
    wait_all(out.at[others], send_sems.at[1])
    wait_all(out.at[others], recv_sems.at[1])


def spread(slices, own):
    return pl.pallas_call(
        spread_kernel,
        name="spread",
        out_shape=(
            jax.ShapeDtypeStruct(slices.shape, slices.dtype),
            jax.ShapeDtypeStruct((DEVS, *own.shape), own.dtype),
        ),
        in_specs=[ANY_SPEC, ANY_SPEC],
        out_specs=(ANY_SPEC, ANY_SPEC),
        scratch_shapes=[pltpu.SemaphoreType.DMA((2,))] * 3,
        compiler_params=pltpu.CompilerParams(
            has_side_effects=True, vmem_limit_bytes=VMEM_LIMIT
        ),
    )(slices, own)


def share_kernel(own, out, send_sem, recv_sem, here_sem):
    spot = position()
    me = flat(spot)
    mine = pltpu.make_async_copy(own, out.at[me], here_sem)
    mine.start()

    def send(i, carry):
        pltpu.make_async_remote_copy(
            src_ref=own,
            dst_ref=out.at[me],
            send_sem=send_sem,
            recv_sem=recv_sem,
            device_id=tuple(partner(spot, i)),
            device_id_type=MESH_ID,
        ).start()
        return carry

    lax.fori_loop(1, DEVS, send, 0)
    mine.wait()
    others = pl.ds(0, DEVS - 1)
    wait_all(out.at[others], send_sem)
    wait_all(out.at[others], recv_sem)


def share(own):
    return pl.pallas_call(
        share_kernel,
        name="share",
        out_shape=jax.ShapeDtypeStruct((DEVS, *own.shape), own.dtype),
        in_specs=[ANY_SPEC],
        out_specs=ANY_SPEC,
        scratch_shapes=[pltpu.SemaphoreType.DMA] * 3,
        compiler_params=pltpu.CompilerParams(has_side_effects=True, vmem_limit_bytes=VMEM_LIMIT),
    )(own)


def pack_kernel(meta, starts, slices, out, table, windows, sem):
    q = meta[1]

    def kind_of(k):
        return lax.bitwise_and(q - lax.shift_right_arithmetic(k, 4), 7)

    def fill(k, carry):
        which = kind_of(k)
        kind = lax.bitwise_and(which, 3)
        m = lax.shift_right_arithmetic(which, 2)

        def owner(row_tile, col_tile):
            return lax.bitwise_and(row_tile, 15) * 8 + lax.bitwise_and(col_tile, 7)

        far = k + kind
        upper = slices[owner(k, far), m, 0].astype(F32)
        lower = slices[owner(far, k), m, 1].astype(F32)
        table[2 * k] = encode(jnp.where(kind > 0, upper + lower, upper))
        near = k - 7 + kind
        upper = slices[owner(near, k), m, 0].astype(F32)
        lower = slices[owner(k, near), m, 1].astype(F32)
        table[2 * k + 1] = encode(upper + lower)
        return carry

    lax.fori_loop(0, NT, fill, 0, unroll=4)

    def window(a, carry):
        for t in range(KT):
            kind = lax.bitwise_and(kind_of(a + t), 3)
            wraps = (kind > 0) & (t + kind > KT - 1)
            windows[a, t] = table[2 * (a + t) + wraps.astype(I32)]
        return carry

    lax.fori_loop(0, STARTS, window, 0, unroll=2)

    def send(d, carry):
        for b in range(2):
            pltpu.make_async_copy(windows.at[starts[2 * d + b]], out.at[b, d], sem).start()
        return carry

    lax.fori_loop(0, DEVS, send, 0, unroll=4)
    pltpu.make_async_copy(out, out, sem).wait()


def pack(meta, starts, slices):
    return pl.pallas_call(
        pack_kernel,
        name="pack",
        out_shape=jax.ShapeDtypeStruct((2, DEVS, KT, 8, TILE), I16),
        in_specs=[SMEM_SPEC, SMEM_SPEC, VMEM_SPEC],
        out_specs=ANY_SPEC,
        scratch_shapes=[
            pltpu.VMEM((2 * NT, 8, TILE), I16),
            pltpu.VMEM((STARTS, KT, 8, TILE), I16),
            pltpu.SemaphoreType.DMA,
        ],
        compiler_params=pltpu.CompilerParams(vmem_limit_bytes=VMEM_LIMIT),
    )(meta, starts, slices)


def harmonics(x, y, z):
    radius_sq = x * x + y * y + z * z
    return [
        None,
        x,
        y,
        z,
        x * y,
        y * z,
        3.0 * z * z - radius_sq,
        x * z,
        x * x - y * y,
    ]


CHUNKS = ((0, 0, 7), (1, 0, 4), (1, 4, 7))


def batches_kernel(info, outgoing, basis, offsets, weights, atoms, dens, moments, *scratch):
    arrived = scratch[: len(CHUNKS)]
    values = scratch[len(CHUNKS) : len(CHUNKS) + 2]
    matrix, kept, sums, send_sems, recv_sems, here_sems, basis_sems = scratch[len(CHUNKS) + 2 :]
    spot = position()
    me = flat(spot)
    points = basis.shape[1]

    def own_copy(n):
        b, low, high = CHUNKS[n]
        return pltpu.make_async_copy(
            outgoing.at[b, me, pl.ds(low, high - low)], arrived[n].at[me], here_sems.at[n]
        )

    def basis_copy(b, j):
        return pltpu.make_async_copy(
            basis.at[b, :, pl.ds(j * TILE, TILE)], values[b].at[j], basis_sems.at[b, j]
        )

    for n, (b, low, high) in enumerate(CHUNKS):

        def send(i, carry, n=n, b=b, low=low, high=high):
            to = partner(spot, i)
            pltpu.make_async_remote_copy(
                src_ref=outgoing.at[b, flat(to), pl.ds(low, high - low)],
                dst_ref=arrived[n].at[me],
                send_sem=send_sems.at[n],
                recv_sem=recv_sems.at[n],
                device_id=tuple(to),
                device_id_type=MESH_ID,
            ).start()
            return carry

        lax.fori_loop(1, DEVS, send, 0)
        own_copy(n).start()
        if n < 2:
            for j in range(KT):
                basis_copy(n, j).start()

    others = pl.ds(0, DEVS - 1)
    rows = points // TILE
    place = lax.broadcasted_iota(I32, (rows, TILE), 0) * TILE + lax.broadcasted_iota(
        I32, (rows, TILE), 1
    )
    for n, (b, low, high) in enumerate(CHUNKS):
        first = low == 0
        last = high == KT
        if first:
            for j in range(KT):
                basis_copy(b, j).wait()
        own_copy(n).wait()
        wait_all(arrived[n].at[others], recv_sems.at[n])
        for t in range(low, high):
            turn = lax.shift_right_arithmetic(info[b, 0] + t, 4)
            for kind in range(4):
                live = (info[b, 3 + KT + t] * info[b, 3 + KT + (t + kind) % KT]).astype(F32)
                for m in range(2):
                    q = lax.bitwise_and(kind + 4 * m + turn, 7)
                    codes = [arrived[n][s * N_COL + q, t - low] for s in range(N_ROW)]
                    value = decode(jnp.concatenate(codes, axis=0)) * live
                    upper = value.astype(BF16)
                    lower = (value - upper.astype(F32)).astype(BF16)
                    columns = pl.ds(m * TILE, TILE)
                    matrix[t, pl.ds(kind * TILE, TILE), columns] = upper
                    matrix[t, pl.ds((4 + kind) * TILE, TILE), columns] = lower
        at = [info[b, 3 + t] for t in range(KT)]

        def step(block, carry, b=b, low=low, high=high, first=first, last=last, at=at):
            span = pl.ds(pl.multiple_of(block * BLOCK, BLOCK), BLOCK)
            total = None if first else kept[span, :]
            for t in range(low, high):
                left = jnp.concatenate(
                    [values[b][at[(t + i) % KT], span, :] for i in range(4)], axis=1
                )
                product = jnp.dot(
                    left, matrix[t, pl.ds(0, 4 * TILE), :], preferred_element_type=F32
                ) + jnp.dot(
                    left, matrix[t, pl.ds(4 * TILE, 4 * TILE), :], preferred_element_type=F32
                )
                own = left[:, :TILE].astype(F32)
                term = product * jnp.concatenate([own, own], axis=1)
                total = term if total is None else total + term
            if not last:
                kept[span, :] = total
            else:
                for m in range(2):
                    for i in range(GROUPS):
                        part = total[i * TILE : (i + 1) * TILE, m * TILE : (m + 1) * TILE]
                        dens[m, b, pl.ds(block * GROUPS + i, 1), :] = jnp.sum(
                            part.T, axis=0, keepdims=True
                        )
            return carry

        lax.fori_loop(0, points // BLOCK, step, 0)
        if not last:
            continue
        inside = place < info[b, 1]
        harmonic = harmonics(offsets[0, b], offsets[1, b], offsets[2, b])
        weight = weights[b]
        factors = [weight] + [weight * item for item in harmonic[1:]]
        atom = atoms[b]
        hits = [atom == lax.bitwise_and(info[b, 2] + j, ATOMS - 1) for j in range(8)]
        sums[...] = jnp.zeros(sums.shape, F32)
        for m in range(2):
            value = jnp.where(inside, dens[m, b], 0.0)
            dens[m, b] = value
            for h in range(9):
                term = value * factors[h]
                for j in range(8):
                    picked = jnp.where(hits[j], term, 0.0)
                    sums[pl.ds(j * 18 + m * 9 + h, 1), :] = jnp.sum(
                        picked, axis=0, keepdims=True
                    )
        for i in range(2):
            part = sums[pl.ds(i * TILE, TILE), :]
            moments[b, pl.ds(i, 1), :] = jnp.sum(part.T, axis=0, keepdims=True)
    for n in range(len(CHUNKS)):
        wait_all(arrived[n].at[others], send_sems.at[n])


def batches(info, outgoing, basis, offsets, weights, atoms):
    points = basis.shape[1]
    rows = points // TILE
    return pl.pallas_call(
        batches_kernel,
        name="batches",
        out_shape=(
            jax.ShapeDtypeStruct((2, 2, rows, TILE), F32),
            jax.ShapeDtypeStruct((2, 2, TILE), F32),
        ),
        in_specs=[SMEM_SPEC, ANY_SPEC, ANY_SPEC, VMEM_SPEC, VMEM_SPEC, VMEM_SPEC],
        out_specs=(VMEM_SPEC, VMEM_SPEC),
        scratch_shapes=[
            *(pltpu.VMEM((DEVS, high - low, 8, TILE), I16) for _, low, high in CHUNKS),
            pltpu.VMEM((KT, points, TILE), BF16),
            pltpu.VMEM((KT, points, TILE), BF16),
            pltpu.VMEM((KT, 8 * TILE, 2 * TILE), BF16),
            pltpu.VMEM((points, 2 * TILE), F32),
            pltpu.VMEM((2 * TILE, TILE), F32),
            pltpu.SemaphoreType.DMA((len(CHUNKS),)),
            pltpu.SemaphoreType.DMA((len(CHUNKS),)),
            pltpu.SemaphoreType.DMA((len(CHUNKS),)),
            pltpu.SemaphoreType.DMA((2, KT)),
        ],
        compiler_params=pltpu.CompilerParams(has_side_effects=True, vmem_limit_bytes=VMEM_LIMIT),
    )(info, outgoing, basis, offsets, weights, atoms)


def local(
    density_first,
    density_second,
    basis,
    tile_list,
    tile_count,
    point_count,
    offsets,
    weights,
    atom_of_point,
):
    points = basis.shape[1]
    rows = points // TILE
    my_row = lax.axis_index(ROW).astype(I32)
    my_col = lax.axis_index(COL).astype(I32)
    device = my_row * N_COL + my_col
    meta = jnp.stack([my_row, my_col])
    own_start = jnp.min(tile_list, axis=1)
    place = jnp.argsort(tile_list, axis=1).astype(I32)
    live = (place < tile_count[:, None]).astype(I32)
    base = (2 * device + jnp.arange(2, dtype=I32)) * 4 % ATOMS
    info = jnp.concatenate(
        [own_start[:, None], point_count[:, None], base[:, None], place, live], axis=1
    )
    offsets = offsets.reshape(3, 2, rows, TILE)
    weights = weights.reshape(2, rows, TILE)
    atom_of_point = atom_of_point.reshape(2, rows, TILE)

    slices = extract(meta, density_first, density_second)
    slices, starts = spread(
        slices.reshape(DEVS, 2, 2, 8, TILE), jnp.pad(own_start, (0, TILE - 2))[None]
    )
    outgoing = pack(meta, starts[:, 0, :2].reshape(-1), slices)
    dens, moments = batches(info, outgoing, basis, offsets, weights, atom_of_point)
    density = dens.reshape(2, 2, points)
    moments = moments.reshape(2, -1)[:, : 8 * 18]
    half = 4 * 18
    own = jnp.concatenate(
        [moments[0][:half], moments[0][half:] + moments[1][:half], moments[1][half:]]
    )
    spare = jnp.zeros((2 * TILE - 3 * half,), F32)
    own = jnp.concatenate([own, spare])
    everyone = share(own[None])[:, 0]
    main = everyone[:, : 2 * half]
    extra = jnp.roll(everyone[:, 2 * half : 3 * half], 1, axis=0)
    whole = main + jnp.concatenate([extra, jnp.zeros_like(extra)], axis=1)
    whole = whole.reshape(ATOMS, 18).T.reshape(2, 9, ATOMS)
    return (density, whole)


def solution(mesh):
    torus = Mesh(mesh.devices.reshape(4, 4, 4, 2), ("row_0", "row_1", "col_0", "col_1"))
    in_specs = (
        P(ROW, COL),
        P(ROW, COL),
        P(ROW_COL, None, None),
        P(ROW_COL, None),
        P(ROW_COL),
        P(ROW_COL),
        P(None, ROW_COL, None),
        P(ROW_COL, None),
        P(ROW_COL, None),
    )
    out_specs = (P(None, ROW_COL, None), P())
    return jax.shard_map(local, mesh=torus, in_specs=in_specs, out_specs=out_specs, check_vma=False)
```

```python
import functools

import jax
import jax.numpy as jnp
from jax import lax
from jax.experimental import pallas as pl
from jax.experimental.pallas import tpu as pltpu
from jax.sharding import Mesh
from jax.sharding import PartitionSpec as P

TILE = 128
ATOMS = 1024
ROW = ("row_0", "row_1")
COL = ("col_0", "col_1")
ROW_COL = ("row_0", "row_1", "col_0", "col_1")
KT = 7
N_ROW = 16
N_COL = 8
DEVS = N_ROW * N_COL
NT = 96
STARTS = NT - KT + 1
LOCAL_T = NT // N_ROW
LOCAL_U = NT // N_COL
BLOCK = 512
GROUPS = BLOCK // TILE
F32 = jnp.float32
BF16 = jnp.bfloat16
I16 = jnp.int16
I32 = jnp.int32
VMEM_LIMIT = 60 * 1024 * 1024
MESH_ID = pl.DeviceIdType.MESH
SMEM_SPEC = pl.BlockSpec(memory_space=pltpu.SMEM)
VMEM_SPEC = pl.BlockSpec(memory_space=pltpu.VMEM)
ANY_SPEC = pl.BlockSpec(memory_space=pl.ANY)


def encode(value):
    size = jnp.abs(value)
    safe = jnp.maximum(size, 2.0**-38)
    power = jnp.floor(jnp.log2(safe))
    code = (power + 37.0) * 1024.0 + safe * jnp.exp2(10.0 - power)
    code = jnp.clip(jnp.floor(code + 0.5), 0.0, 32767.0)
    code = jnp.where(size >= 2.0**-38, code, 0.0)
    code = jnp.where(value < 0.0, -code, code)
    return code.astype(I32).astype(I16)


def decode(code):
    code = code.astype(I32)
    size = jnp.abs(code)
    power = lax.shift_right_logical(size, 10).astype(F32)
    fraction = (lax.bitwise_and(size, 1023) + 1024).astype(F32)
    value = fraction * jnp.exp2(power - 48.0)
    value = jnp.where(size > 0, value, 0.0)
    return jnp.where(code < 0, -value, value)


def harmonics(x, y, z):
    radius_sq = x * x + y * y + z * z
    return [
        None,
        x,
        y,
        z,
        x * y,
        y * z,
        3.0 * z * z - radius_sq,
        x * z,
        x * x - y * y,
    ]


CHUNKS = ((0, 0, 4), (0, 4, 7), (1, 0, 4), (1, 4, 6), (1, 6, 7))
OTHERS = pl.ds(0, DEVS - 1)


def flat(spot):
    return ((spot[0] * 4 + spot[1]) * 4 + spot[2]) * 2 + spot[3]


def wait_all(ref, sem):
    pltpu.make_async_copy(ref, ref, sem).wait()


def to_everyone(spot, send):
    z, x, y, core = spot
    way = 1 - 2 * core
    zs = [(z + way * k + 4) % 4 for k in range(4)]
    xs = [(x + way * k + 4) % 4 for k in range(4)]
    first = tuple((y + way * k + 4) % 4 for k in range(4))
    both = [core, 1 - core]
    for turn in range(2):

        def step(i, ys, turn=turn):
            for n in range(16):
                b = n % 4
                a = (n // 4 + b) % 4
                partner = (zs[a], xs[b], ys[(a + b) % 4], both[(turn + a) % 2])
                if n == 0 and turn == 0:

                    @pl.when(i > 0)
                    def _(partner=partner):
                        send(partner)
                else:
                    send(partner)
            return (*ys[1:], ys[0])

        lax.fori_loop(0, 4, step, first)


def remote(source, target, send_sem, recv_sem, partner):
    pltpu.make_async_remote_copy(
        src_ref=source,
        dst_ref=target,
        send_sem=send_sem,
        recv_sem=recv_sem,
        device_id=partner,
        device_id_type=MESH_ID,
    ).start()


def extract_tile(r, e, tile, m, ul, t):
    row_tile = r + 16 * t
    if ul == 0:
        d = e
        near = 1 - e // 4
        key = row_tile + d * (1 - near)
        turned = (e >= 1) & (e <= 3)
    else:
        d = 8 - e
        near = (e + 3) // 8
        key = row_tile - d * near
        turned = e <= 4
    kind = near * d + (1 - near) * (7 - d)
    q = (kind + 4 * m + (key + 16) // 16 + 15) % 8
    value = tile.astype(F32)
    value = jnp.where(turned, value.T, value)
    return q, value.reshape(N_ROW, 8, TILE).astype(BF16)


def whole_kernel(
    first,
    second,
    basis,
    tile_list,
    tile_count,
    point_count,
    far_offsets,
    far_weights,
    far_atoms,
    density,
    moments,
    offsets,
    weights,
    atoms,
    tiles,
    banded,
    slices,
    table,
    windows,
    own_starts,
    vector_starts,
    starts,
    outgoing,
    matrix,
    kept,
    geometry,
    labels,
    dens,
    sums,
    own_moments,
    all_moments,
    point_sems,
    tile_sems,
    basis_sems,
    here_sems,
    send_sems,
    recv_sems,
    *buffers,
):
    arrived = buffers[: len(CHUNKS)]
    values = buffers[len(CHUNKS) :]
    spot = [lax.axis_index(name) for name in ROW_COL]
    me = flat(spot)
    r = spot[0] * 4 + spot[1]
    c = spot[2] * 2 + spot[3]
    e = (c - r + 16) % 8
    points = basis.shape[1]
    rows = points // TILE
    point_copies = [
        pltpu.make_async_copy(source, target, point_sems.at[k])
        for k, (source, target) in enumerate(
            [(far_offsets, offsets), (far_weights, weights), (far_atoms, atoms)]
        )
    ]

    def tile_copy(m, ul, t):
        column = (r + 16 * t + e - 8 * ul - c + 64) // 8 - 8
        column = jnp.minimum(jnp.maximum(column, 0), LOCAL_U - 1)
        source = (first, second)[m]
        return pltpu.make_async_copy(
            source.at[pl.ds(t * TILE, TILE), pl.ds(pl.multiple_of(column * TILE, TILE), TILE)],
            tiles.at[m, ul, t],
            tile_sems.at[m, ul, t],
        )

    def basis_copy(b, j):
        return pltpu.make_async_copy(
            basis.at[b, :, pl.ds(j * TILE, TILE)], values[b].at[j], basis_sems.at[b, j]
        )

    todo = [(m, ul, t) for m in range(2) for ul in range(2) for t in range(LOCAL_T)]
    for item in todo:
        tile_copy(*item).start()
    for copy in point_copies:
        copy.start()
    barrier = pltpu.get_barrier_semaphore()
    to_everyone(
        spot,
        lambda partner: pl.semaphore_signal(
            barrier, inc=1, device_id=partner, device_id_type=MESH_ID
        ),
    )

    listed = [[tile_list[b, p] for p in range(KT)] for b in range(2)]
    begin = [functools.reduce(jnp.minimum, one) for one in listed]
    place = [
        [
            jnp.minimum(
                sum(jnp.where(listed[b][p] == begin[b] + t, p, 0) for p in range(KT)), KT - 1
            )
            for t in range(KT)
        ]
        for b in range(2)
    ]
    live = [[(place[b][t] < tile_count[b]).astype(F32) for t in range(KT)] for b in range(2)]
    lane = lax.broadcasted_iota(I32, (1, TILE), 1)
    own_starts[...] = jnp.where(lane == 0, begin[0], begin[1])

    banded[...] = jnp.zeros(banded.shape, BF16)
    for m, ul, t in todo:
        tile_copy(m, ul, t).wait()
        q, value = extract_tile(r, e, tiles[m, ul, t], m, ul, t)
        banded[:, q, ul, m] = value
    pl.semaphore_wait(barrier, DEVS - 1)

    for ul in range(2):

        @pl.when((e <= 6) if ul == 0 else (e >= 2))
        def _(ul=ul):
            to_everyone(
                spot,
                lambda to: remote(
                    banded.at[to[0] * 4 + to[1], to[2] * 2 + to[3], ul],
                    slices.at[me, ul],
                    send_sems.at[1 + ul],
                    recv_sems.at[1 + ul],
                    to,
                ),
            )

    to_everyone(
        spot,
        lambda to: remote(
            own_starts, vector_starts.at[me], send_sems.at[0], recv_sems.at[0], to
        ),
    )
    vector_starts[me] = own_starts[...]
    slices[me] = banded[r, c]
    for b in range(2):
        for j in range(KT):
            basis_copy(b, j).start()
    for copy in point_copies:
        copy.wait()
    for b in range(2):
        for i in range(rows):
            lanes = pl.ds(i * TILE, TILE)
            for k in range(3):
                geometry[k, b, pl.ds(i, 1), :] = offsets[k, pl.ds(b, 1), lanes]
            geometry[3, b, pl.ds(i, 1), :] = weights[pl.ds(b, 1), lanes]
            labels[b, pl.ds(i, 1), :] = atoms[pl.ds(b, 1), lanes]
    wait_all(vector_starts.at[OTHERS], recv_sems.at[0])
    scalars = pltpu.make_async_copy(vector_starts, starts, here_sems.at[0])
    scalars.start()
    scalars.wait()
    for ul in range(2):
        senders = (112, 96)[ul]
        takes_part = (e <= 6) if ul == 0 else (e >= 2)

        @pl.when(takes_part)
        def _(ul=ul, senders=senders):
            wait_all(slices.at[pl.ds(0, senders - 1), ul], recv_sems.at[1 + ul])

        @pl.when(jnp.logical_not(takes_part))
        def _(ul=ul, senders=senders):
            wait_all(slices.at[pl.ds(0, senders), ul], recv_sems.at[1 + ul])

    def kind_of(k):
        return lax.bitwise_and(c - lax.shift_right_logical(k, 4), 7)

    def owner(row_tile, col_tile):
        return lax.bitwise_and(row_tile, 15) * 8 + lax.bitwise_and(col_tile, 7)

    def fill(k, carry):
        which = kind_of(k)
        kind = lax.bitwise_and(which, 3)
        m = lax.shift_right_logical(which, 2)
        far = k + kind
        paired = lax.shift_right_logical(kind + 3, 2)
        upper = slices[owner(k, far), 0, m].astype(F32)
        lower = slices[owner(far, k), paired, m].astype(F32)
        table[2 * k] = encode(upper + lower * paired.astype(F32))
        near = k + 9 + kind + (1 - paired)
        upper = slices[owner(near, k), 0, m].astype(F32)
        lower = slices[owner(k, near + 8), 1, m].astype(F32)
        table[2 * k + 1] = encode(upper + lower)
        return carry

    lax.fori_loop(0, NT, fill, 0, unroll=8)

    def window(a, carry):
        for t in range(KT):
            kind = lax.bitwise_and(kind_of(a + t), 3)
            wraps = lax.shift_right_logical(t + kind + 1, 3)
            windows[a, t] = table[2 * (a + t) + wraps]
        return carry

    lax.fori_loop(0, STARTS, window, 0, unroll=5)

    for b in range(2):

        def pack(d, carry, b=b):
            outgoing[b, d] = windows[starts[d, 0, b]]
            return carry

        lax.fori_loop(0, DEVS, pack, 0, unroll=8)

    for n, (b, low, high) in enumerate(CHUNKS):
        part = pl.ds(low, high - low)
        to_everyone(
            spot,
            lambda to, n=n, b=b, part=part: remote(
                outgoing.at[b, flat(to), part],
                arrived[n].at[me],
                send_sems.at[3 + n],
                recv_sems.at[3 + n],
                to,
            ),
        )
        arrived[n][me] = outgoing[b, me, part]

    spots = lax.broadcasted_iota(I32, (rows, TILE), 0) * TILE + lax.broadcasted_iota(
        I32, (rows, TILE), 1
    )
    for n, (b, low, high) in enumerate(CHUNKS):
        begins = low == 0
        ends = high == KT
        if begins:
            for j in range(KT):
                basis_copy(b, j).wait()
        wait_all(arrived[n].at[OTHERS], recv_sems.at[3 + n])
        for t in range(low, high):
            turn = lax.shift_right_arithmetic(begin[b] + t, 4)
            for kind in range(4):
                alive = live[b][t] * live[b][(t + kind) % KT]
                for m in range(2):
                    q = lax.bitwise_and(kind + 4 * m + turn, 7)
                    codes = [arrived[n][s * N_COL + q, t - low] for s in range(N_ROW)]
                    value = decode(jnp.concatenate(codes, axis=0)) * alive
                    upper = value.astype(BF16)
                    lower = (value - upper.astype(F32)).astype(BF16)
                    columns = pl.ds(m * TILE, TILE)
                    matrix[t, pl.ds(kind * TILE, TILE), columns] = upper
                    matrix[t, pl.ds((4 + kind) * TILE, TILE), columns] = lower

        def step(block, carry, b=b, low=low, high=high, begins=begins, ends=ends):
            span = pl.ds(pl.multiple_of(block * BLOCK, BLOCK), BLOCK)
            total = None if begins else kept[span, :]
            for t in range(low, high):
                left = jnp.concatenate(
                    [values[b][place[b][(t + i) % KT], span, :] for i in range(4)], axis=1
                )
                product = jnp.dot(
                    left, matrix[t, pl.ds(0, 4 * TILE), :], preferred_element_type=F32
                ) + jnp.dot(
                    left, matrix[t, pl.ds(4 * TILE, 4 * TILE), :], preferred_element_type=F32
                )
                own = left[:, :TILE].astype(F32)
                term = product * jnp.concatenate([own, own], axis=1)
                total = term if total is None else total + term
            if not ends:
                kept[span, :] = total
            else:
                for m in range(2):
                    for i in range(GROUPS):
                        part = total[i * TILE : (i + 1) * TILE, m * TILE : (m + 1) * TILE]
                        dens[m, b, pl.ds(block * GROUPS + i, 1), :] = jnp.sum(
                            part.T, axis=0, keepdims=True
                        )
            return carry

        lax.fori_loop(0, points // BLOCK, step, 0)
        if not ends:
            continue
        inside = spots < point_count[b]
        harmonic = harmonics(geometry[0, b], geometry[1, b], geometry[2, b])
        weight = geometry[3, b]
        factors = [weight] + [weight * item for item in harmonic[1:]]
        base = (me * 8 + b * 4) % ATOMS
        hits = [labels[b] == (base + j) % ATOMS for j in range(8)]
        if b == 0:
            sums[...] = jnp.zeros(sums.shape, F32)
        for m in range(2):
            value = jnp.where(inside, dens[m, b], 0.0)
            dens[m, b] = value
            for h in range(9):
                term = value * factors[h]
                for j in range(8):
                    line = jnp.sum(jnp.where(hits[j], term, 0.0), axis=0, keepdims=True)
                    at = pl.ds((j + 4 * b) * 18 + m * 9 + h, 1)
                    sums[at, :] = line if b == 0 or j >= 4 else sums[at, :] + line
    for i in range(2):
        part = sums[pl.ds(i * TILE, TILE), :]
        own_moments[pl.ds(i, 1), :] = jnp.sum(part.T, axis=0, keepdims=True)
    for m in range(2):
        for b in range(2):
            for i in range(rows):
                density[m, pl.ds(b, 1), pl.ds(i * TILE, TILE)] = dens[m, b, pl.ds(i, 1), :]
    last = 3 + len(CHUNKS)
    to_everyone(
        spot,
        lambda to: remote(
            own_moments, all_moments.at[me], send_sems.at[last], recv_sems.at[last], to
        ),
    )
    all_moments[me] = own_moments[...]
    wait_all(vector_starts.at[OTHERS], send_sems.at[0])
    for ul in range(2):

        @pl.when((e <= 6) if ul == 0 else (e >= 2))
        def _(ul=ul):
            wait_all(slices.at[OTHERS, ul], send_sems.at[1 + ul])

    for n in range(len(CHUNKS)):
        wait_all(arrived[n].at[OTHERS], send_sems.at[3 + n])
    wait_all(all_moments.at[OTHERS], send_sems.at[last])
    wait_all(all_moments.at[OTHERS], recv_sems.at[last])
    moments[...] = all_moments[...]


def whole(first, second, basis, tile_list, tile_count, point_count, offsets, weights, atoms):
    points = basis.shape[1]
    rows = points // TILE
    count = 4 + len(CHUNKS)
    return pl.pallas_call(
        whole_kernel,
        name="whole",
        out_shape=(
            jax.ShapeDtypeStruct((2, 2, points), F32),
            jax.ShapeDtypeStruct((DEVS, 2, TILE), F32),
        ),
        in_specs=[ANY_SPEC] * 3 + [SMEM_SPEC] * 3 + [ANY_SPEC] * 3,
        out_specs=(VMEM_SPEC, VMEM_SPEC),
        scratch_shapes=[
            pltpu.VMEM(offsets.shape, F32),
            pltpu.VMEM(weights.shape, F32),
            pltpu.VMEM(atoms.shape, I32),
            pltpu.VMEM((2, 2, LOCAL_T, TILE, TILE), BF16),
            pltpu.VMEM((N_ROW, N_COL, 2, 2, 8, TILE), BF16),
            pltpu.VMEM((DEVS, 2, 2, 8, TILE), BF16),
            pltpu.VMEM((2 * NT, 8, TILE), I16),
            pltpu.VMEM((STARTS, KT, 8, TILE), I16),
            pltpu.VMEM((1, TILE), I32),
            pltpu.VMEM((DEVS, 1, TILE), I32),
            pltpu.SMEM((DEVS, 1, TILE), I32),
            pltpu.VMEM((2, DEVS, KT, 8, TILE), I16),
            pltpu.VMEM((KT, 8 * TILE, 2 * TILE), BF16),
            pltpu.VMEM((points, 2 * TILE), F32),
            pltpu.VMEM((4, 2, rows, TILE), F32),
            pltpu.VMEM((2, rows, TILE), I32),
            pltpu.VMEM((2, 2, rows, TILE), F32),
            pltpu.VMEM((2 * TILE, TILE), F32),
            pltpu.VMEM((2, TILE), F32),
            pltpu.VMEM((DEVS, 2, TILE), F32),
            pltpu.SemaphoreType.DMA((3,)),
            pltpu.SemaphoreType.DMA((2, 2, LOCAL_T)),
            pltpu.SemaphoreType.DMA((2, KT)),
            pltpu.SemaphoreType.DMA((1,)),
            pltpu.SemaphoreType.DMA((count,)),
            pltpu.SemaphoreType.DMA((count,)),
            *(pltpu.VMEM((DEVS, high - low, 8, TILE), I16) for _, low, high in CHUNKS),
            pltpu.VMEM((KT, points, TILE), BF16),
            pltpu.VMEM((KT, points, TILE), BF16),
        ],
        compiler_params=pltpu.CompilerParams(
            collective_id=0, has_side_effects=True, vmem_limit_bytes=VMEM_LIMIT
        ),
    )(first, second, basis, tile_list, tile_count, point_count, offsets, weights, atoms)


def local(
    density_first,
    density_second,
    basis,
    tile_list,
    tile_count,
    point_count,
    offsets,
    weights,
    atom_of_point,
):
    density, shared = whole(
        density_first,
        density_second,
        basis,
        tile_list,
        tile_count,
        point_count,
        offsets,
        weights,
        atom_of_point,
    )
    everyone = shared.reshape(DEVS, 2 * TILE)
    half = 4 * 18
    main = everyone[:, : 2 * half]
    extra = jnp.roll(everyone[:, 2 * half : 3 * half], 1, axis=0)
    whole_moments = main + jnp.concatenate([extra, jnp.zeros_like(extra)], axis=1)
    return (density, whole_moments.reshape(ATOMS, 18).T.reshape(2, 9, ATOMS))


def solution(mesh):
    torus = Mesh(mesh.devices.reshape(4, 4, 4, 2), ("row_0", "row_1", "col_0", "col_1"))
    in_specs = (
        P(ROW, COL),
        P(ROW, COL),
        P(ROW_COL, None, None),
        P(ROW_COL, None),
        P(ROW_COL),
        P(ROW_COL),
        P(None, ROW_COL, None),
        P(ROW_COL, None),
        P(ROW_COL, None),
    )
    out_specs = (P(None, ROW_COL, None), P())
    return jax.shard_map(local, mesh=torus, in_specs=in_specs, out_specs=out_specs, check_vma=False)
```

```python
import functools

import jax
import jax.numpy as jnp
from jax import lax
from jax.experimental import pallas as pl
from jax.experimental.pallas import tpu as pltpu
from jax.sharding import Mesh
from jax.sharding import PartitionSpec as P

TILE = 128
ATOMS = 1024
ROW = ("row_0", "row_1")
COL = ("col_0", "col_1")
ROW_COL = ("row_0", "row_1", "col_0", "col_1")
KT = 7
N_ROW = 16
N_COL = 8
DEVS = N_ROW * N_COL
NT = 96
STARTS = NT - KT + 1
LOCAL_T = NT // N_ROW
LOCAL_U = NT // N_COL
BLOCK = 1024
GROUPS = BLOCK // TILE
F32 = jnp.float32
BF16 = jnp.bfloat16
I16 = jnp.int16
I32 = jnp.int32
F8 = jnp.float8_e5m2
LOW_SCALE = 2.0**30
BASIS_SCALE = 2.0**13
LOW_UNSCALE = 2.0**-43
VMEM_LIMIT = 60 * 1024 * 1024
MESH_ID = pl.DeviceIdType.MESH
SMEM_SPEC = pl.BlockSpec(memory_space=pltpu.SMEM)
VMEM_SPEC = pl.BlockSpec(memory_space=pltpu.VMEM)
ANY_SPEC = pl.BlockSpec(memory_space=pl.ANY)


def encode(value):
    size = jnp.abs(value)
    safe = jnp.maximum(size, 2.0**-38)
    power = jnp.floor(jnp.log2(safe))
    code = (power + 37.0) * 1024.0 + safe * jnp.exp2(10.0 - power)
    code = jnp.clip(jnp.floor(code + 0.5), 0.0, 32767.0)
    code = jnp.where(size >= 2.0**-38, code, 0.0)
    code = jnp.where(value < 0.0, -code, code)
    return code.astype(I32).astype(I16)


def decode(code):
    code = code.astype(I32)
    size = jnp.abs(code)
    power = lax.shift_right_logical(size, 10).astype(F32)
    fraction = (lax.bitwise_and(size, 1023) + 1024).astype(F32)
    value = fraction * jnp.exp2(power - 48.0)
    value = jnp.where(size > 0, value, 0.0)
    return jnp.where(code < 0, -value, value)


def harmonics(x, y, z):
    radius_sq = x * x + y * y + z * z
    return [
        None,
        x,
        y,
        z,
        x * y,
        y * z,
        3.0 * z * z - radius_sq,
        x * z,
        x * x - y * y,
    ]


CHUNKS = ((0, 0, 4), (0, 4, 7), (1, 0, 4), (1, 4, 6), (1, 6, 7))
OTHERS = pl.ds(0, DEVS - 1)


def flat(spot):
    return ((spot[0] * 4 + spot[1]) * 4 + spot[2]) * 2 + spot[3]


def wait_all(ref, sem):
    pltpu.make_async_copy(ref, ref, sem).wait()


def to_everyone(spot, send):
    z, x, y, core = spot
    way = 1 - 2 * core
    zs = [(z + way * k + 4) % 4 for k in range(4)]
    xs = [(x + way * k + 4) % 4 for k in range(4)]
    first = tuple((y + way * k + 4) % 4 for k in range(4))
    both = [core, 1 - core]
    for turn in range(2):

        def step(i, ys, turn=turn):
            for n in range(16):
                b = n % 4
                a = (n // 4 + b) % 4
                partner = (zs[a], xs[b], ys[(a + b) % 4], both[(turn + a) % 2])
                if n == 0 and turn == 0:

                    @pl.when(i > 0)
                    def _(partner=partner):
                        send(partner)
                else:
                    send(partner)
            return (*ys[1:], ys[0])

        lax.fori_loop(0, 4, step, first)


def remote(source, target, send_sem, recv_sem, partner):
    pltpu.make_async_remote_copy(
        src_ref=source,
        dst_ref=target,
        send_sem=send_sem,
        recv_sem=recv_sem,
        device_id=partner,
        device_id_type=MESH_ID,
    ).start()


def extract_tile(r, e, tile, m, ul, t):
    row_tile = r + 16 * t
    if ul == 0:
        d = e
        near = 1 - e // 4
        key = row_tile + d * (1 - near)
        turned = (e >= 1) & (e <= 3)
    else:
        d = 8 - e
        near = (e + 3) // 8
        key = row_tile - d * near
        turned = e <= 4
    kind = near * d + (1 - near) * (7 - d)
    q = (kind + 4 * m + (key + 16) // 16 + 15) % 8
    value = tile.astype(F32)
    value = jnp.where(turned, value.T, value)
    return q, value.reshape(N_ROW, 8, TILE).astype(BF16)


def whole_kernel(
    first,
    second,
    basis,
    tile_list,
    tile_count,
    point_count,
    far_offsets,
    far_weights,
    far_atoms,
    density,
    moments,
    offsets,
    weights,
    atoms,
    tiles,
    banded,
    slices,
    table,
    windows,
    own_starts,
    vector_starts,
    starts,
    outgoing,
    matrix,
    low_matrix,
    kept,
    geometry,
    labels,
    dens,
    sums,
    own_moments,
    all_moments,
    point_sems,
    tile_sems,
    basis_sems,
    here_sems,
    send_sems,
    recv_sems,
    *buffers,
):
    arrived = buffers[: len(CHUNKS)]
    values = buffers[len(CHUNKS) : len(CHUNKS) + 2]
    low_values = buffers[len(CHUNKS) + 2 :]
    spot = [lax.axis_index(name) for name in ROW_COL]
    me = flat(spot)
    r = spot[0] * 4 + spot[1]
    c = spot[2] * 2 + spot[3]
    e = (c - r + 16) % 8
    points = basis.shape[1]
    rows = points // TILE
    point_copies = [
        pltpu.make_async_copy(source, target, point_sems.at[k])
        for k, (source, target) in enumerate(
            [(far_offsets, offsets), (far_weights, weights), (far_atoms, atoms)]
        )
    ]

    def tile_copy(m, ul, t):
        column = (r + 16 * t + e - 8 * ul - c + 64) // 8 - 8
        column = jnp.minimum(jnp.maximum(column, 0), LOCAL_U - 1)
        source = (first, second)[m]
        return pltpu.make_async_copy(
            source.at[pl.ds(t * TILE, TILE), pl.ds(pl.multiple_of(column * TILE, TILE), TILE)],
            tiles.at[m, ul, t],
            tile_sems.at[m, ul, t],
        )

    def basis_copy(b, j):
        return pltpu.make_async_copy(
            basis.at[b, :, pl.ds(j * TILE, TILE)], values[b].at[j], basis_sems.at[b, j]
        )

    todo = [(m, ul, t) for m in range(2) for ul in range(2) for t in range(LOCAL_T)]
    for item in todo:
        tile_copy(*item).start()
    for copy in point_copies:
        copy.start()
    barrier = pltpu.get_barrier_semaphore()
    to_everyone(
        spot,
        lambda partner: pl.semaphore_signal(
            barrier, inc=1, device_id=partner, device_id_type=MESH_ID
        ),
    )

    listed = [[tile_list[b, p] for p in range(KT)] for b in range(2)]
    begin = [functools.reduce(jnp.minimum, one) for one in listed]
    place = [
        [
            jnp.minimum(
                sum(jnp.where(listed[b][p] == begin[b] + t, p, 0) for p in range(KT)), KT - 1
            )
            for t in range(KT)
        ]
        for b in range(2)
    ]
    live = [[(place[b][t] < tile_count[b]).astype(F32) for t in range(KT)] for b in range(2)]
    lane = lax.broadcasted_iota(I32, (1, TILE), 1)
    own_starts[...] = jnp.where(lane == 0, begin[0], begin[1])

    banded[...] = jnp.zeros(banded.shape, BF16)
    for m, ul, t in todo:
        tile_copy(m, ul, t).wait()
        q, value = extract_tile(r, e, tiles[m, ul, t], m, ul, t)
        banded[:, q, ul, m] = value
    pl.semaphore_wait(barrier, DEVS - 1)

    for ul in range(2):

        @pl.when((e <= 6) if ul == 0 else (e >= 2))
        def _(ul=ul):
            to_everyone(
                spot,
                lambda to: remote(
                    banded.at[to[0] * 4 + to[1], to[2] * 2 + to[3], ul],
                    slices.at[me, ul],
                    send_sems.at[1 + ul],
                    recv_sems.at[1 + ul],
                    to,
                ),
            )

    to_everyone(
        spot,
        lambda to: remote(
            own_starts, vector_starts.at[me], send_sems.at[0], recv_sems.at[0], to
        ),
    )
    vector_starts[me] = own_starts[...]
    slices[me] = banded[r, c]
    for b in range(2):
        for j in range(KT):
            basis_copy(b, j).start()
    for copy in point_copies:
        copy.wait()
    for b in range(2):
        for i in range(rows):
            lanes = pl.ds(i * TILE, TILE)
            for k in range(3):
                geometry[k, b, pl.ds(i, 1), :] = offsets[k, pl.ds(b, 1), lanes]
            geometry[3, b, pl.ds(i, 1), :] = weights[pl.ds(b, 1), lanes]
            labels[b, pl.ds(i, 1), :] = atoms[pl.ds(b, 1), lanes]
    wait_all(vector_starts.at[OTHERS], recv_sems.at[0])
    scalars = pltpu.make_async_copy(vector_starts, starts, here_sems.at[0])
    scalars.start()
    scalars.wait()
    for ul in range(2):
        senders = (112, 96)[ul]
        takes_part = (e <= 6) if ul == 0 else (e >= 2)

        @pl.when(takes_part)
        def _(ul=ul, senders=senders):
            wait_all(slices.at[pl.ds(0, senders - 1), ul], recv_sems.at[1 + ul])

        @pl.when(jnp.logical_not(takes_part))
        def _(ul=ul, senders=senders):
            wait_all(slices.at[pl.ds(0, senders), ul], recv_sems.at[1 + ul])

    def kind_of(k):
        return lax.bitwise_and(c - lax.shift_right_logical(k, 4), 7)

    def owner(row_tile, col_tile):
        return lax.bitwise_and(row_tile, 15) * 8 + lax.bitwise_and(col_tile, 7)

    def fill(k, carry):
        which = kind_of(k)
        kind = lax.bitwise_and(which, 3)
        m = lax.shift_right_logical(which, 2)
        far = k + kind
        paired = lax.shift_right_logical(kind + 3, 2)
        upper = slices[owner(k, far), 0, m].astype(F32)
        lower = slices[owner(far, k), paired, m].astype(F32)
        table[2 * k] = encode(upper + lower * paired.astype(F32))
        near = k + 9 + kind + (1 - paired)
        upper = slices[owner(near, k), 0, m].astype(F32)
        lower = slices[owner(k, near + 8), 1, m].astype(F32)
        table[2 * k + 1] = encode(upper + lower)
        return carry

    lax.fori_loop(0, NT, fill, 0, unroll=8)

    def window(a, carry):
        for t in range(KT):
            kind = lax.bitwise_and(kind_of(a + t), 3)
            wraps = lax.shift_right_logical(t + kind + 1, 3)
            windows[a, t] = table[2 * (a + t) + wraps]
        return carry

    lax.fori_loop(0, STARTS, window, 0, unroll=5)

    for b in range(2):

        def pack(d, carry, b=b):
            outgoing[b, d] = windows[starts[d, 0, b]]
            return carry

        lax.fori_loop(0, DEVS, pack, 0, unroll=8)

    for n, (b, low, high) in enumerate(CHUNKS):
        part = pl.ds(low, high - low)
        to_everyone(
            spot,
            lambda to, n=n, b=b, part=part: remote(
                outgoing.at[b, flat(to), part],
                arrived[n].at[me],
                send_sems.at[3 + n],
                recv_sems.at[3 + n],
                to,
            ),
        )
        arrived[n][me] = outgoing[b, me, part]

    spots = lax.broadcasted_iota(I32, (rows, TILE), 0) * TILE + lax.broadcasted_iota(
        I32, (rows, TILE), 1
    )
    for n, (b, low, high) in enumerate(CHUNKS):
        begins = low == 0
        ends = high == KT
        if n == 0:
            for each in range(2):
                for j in range(KT):
                    basis_copy(each, j).wait()

                    def narrow(i, carry, each=each, j=j):
                        span = pl.ds(pl.multiple_of(i * BLOCK, BLOCK), BLOCK)
                        value = values[each][j, span, :].astype(F32) * BASIS_SCALE
                        low_values[each][j, span, :] = value.astype(F8)
                        return carry

                    lax.fori_loop(0, points // BLOCK, narrow, 0)
        wait_all(arrived[n].at[OTHERS], recv_sems.at[3 + n])
        for t in range(low, high):
            turn = lax.shift_right_arithmetic(begin[b] + t, 4)
            for kind in range(4):
                alive = live[b][t] * live[b][(t + kind) % KT]
                for m in range(2):
                    q = lax.bitwise_and(kind + 4 * m + turn, 7)
                    codes = [arrived[n][s * N_COL + q, t - low] for s in range(N_ROW)]
                    value = decode(jnp.concatenate(codes, axis=0)) * alive
                    upper = value.astype(BF16)
                    lower = (value - upper.astype(F32)) * LOW_SCALE
                    columns = pl.ds(m * TILE, TILE)
                    matrix[t, pl.ds(kind * TILE, TILE), columns] = upper
                    low_matrix[t, pl.ds(kind * TILE, TILE), columns] = lower.astype(F8)

        def step(block, carry, b=b, low=low, high=high, begins=begins, ends=ends):
            span = pl.ds(pl.multiple_of(block * BLOCK, BLOCK), BLOCK)
            total = None if begins else kept[span, :]
            for t in range(low, high):
                order = [place[b][(t + i) % KT] for i in range(4)]
                left = jnp.concatenate([values[b][p, span, :] for p in order], axis=1)
                low_left = jnp.concatenate([low_values[b][p, span, :] for p in order], axis=1)
                product = jnp.dot(left, matrix[t], preferred_element_type=F32)
                low = jnp.dot(low_left, low_matrix[t], preferred_element_type=F32)
                product = product + low * LOW_UNSCALE
                own = left[:, :TILE].astype(F32)
                term = product * jnp.concatenate([own, own], axis=1)
                total = term if total is None else total + term
            if not ends:
                kept[span, :] = total
            else:
                for m in range(2):
                    for i in range(GROUPS):
                        part = total[i * TILE : (i + 1) * TILE, m * TILE : (m + 1) * TILE]
                        dens[m, b, pl.ds(block * GROUPS + i, 1), :] = jnp.sum(
                            part.T, axis=0, keepdims=True
                        )
            return carry

        lax.fori_loop(0, points // BLOCK, step, 0)
        if not ends:
            continue
        inside = spots < point_count[b]
        harmonic = harmonics(geometry[0, b], geometry[1, b], geometry[2, b])
        weight = geometry[3, b]
        factors = [weight] + [weight * item for item in harmonic[1:]]
        base = (me * 8 + b * 4) % ATOMS
        hits = [labels[b] == (base + j) % ATOMS for j in range(8)]
        if b == 0:
            sums[...] = jnp.zeros(sums.shape, F32)
        for m in range(2):
            value = jnp.where(inside, dens[m, b], 0.0)
            dens[m, b] = value
            for h in range(9):
                term = value * factors[h]
                for j in range(8):
                    line = jnp.sum(jnp.where(hits[j], term, 0.0), axis=0, keepdims=True)
                    at = pl.ds((j + 4 * b) * 18 + m * 9 + h, 1)
                    sums[at, :] = line if b == 0 or j >= 4 else sums[at, :] + line
    for i in range(2):
        part = sums[pl.ds(i * TILE, TILE), :]
        own_moments[pl.ds(i, 1), :] = jnp.sum(part.T, axis=0, keepdims=True)
    for m in range(2):
        for b in range(2):
            for i in range(rows):
                density[m, pl.ds(b, 1), pl.ds(i * TILE, TILE)] = dens[m, b, pl.ds(i, 1), :]
    last = 3 + len(CHUNKS)
    to_everyone(
        spot,
        lambda to: remote(
            own_moments, all_moments.at[me], send_sems.at[last], recv_sems.at[last], to
        ),
    )
    all_moments[me] = own_moments[...]
    wait_all(vector_starts.at[OTHERS], send_sems.at[0])
    for ul in range(2):

        @pl.when((e <= 6) if ul == 0 else (e >= 2))
        def _(ul=ul):
            wait_all(slices.at[OTHERS, ul], send_sems.at[1 + ul])

    for n in range(len(CHUNKS)):
        wait_all(arrived[n].at[OTHERS], send_sems.at[3 + n])
    wait_all(all_moments.at[OTHERS], send_sems.at[last])
    wait_all(all_moments.at[OTHERS], recv_sems.at[last])
    moments[...] = all_moments[...]


def whole(first, second, basis, tile_list, tile_count, point_count, offsets, weights, atoms):
    points = basis.shape[1]
    rows = points // TILE
    count = 4 + len(CHUNKS)
    return pl.pallas_call(
        whole_kernel,
        name="whole",
        out_shape=(
            jax.ShapeDtypeStruct((2, 2, points), F32),
            jax.ShapeDtypeStruct((DEVS, 2, TILE), F32),
        ),
        in_specs=[ANY_SPEC] * 3 + [SMEM_SPEC] * 3 + [ANY_SPEC] * 3,
        out_specs=(VMEM_SPEC, VMEM_SPEC),
        scratch_shapes=[
            pltpu.VMEM(offsets.shape, F32),
            pltpu.VMEM(weights.shape, F32),
            pltpu.VMEM(atoms.shape, I32),
            pltpu.VMEM((2, 2, LOCAL_T, TILE, TILE), BF16),
            pltpu.VMEM((N_ROW, N_COL, 2, 2, 8, TILE), BF16),
            pltpu.VMEM((DEVS, 2, 2, 8, TILE), BF16),
            pltpu.VMEM((2 * NT, 8, TILE), I16),
            pltpu.VMEM((STARTS, KT, 8, TILE), I16),
            pltpu.VMEM((1, TILE), I32),
            pltpu.VMEM((DEVS, 1, TILE), I32),
            pltpu.SMEM((DEVS, 1, TILE), I32),
            pltpu.VMEM((2, DEVS, KT, 8, TILE), I16),
            pltpu.VMEM((KT, 4 * TILE, 2 * TILE), BF16),
            pltpu.VMEM((KT, 4 * TILE, 2 * TILE), F8),
            pltpu.VMEM((points, 2 * TILE), F32),
            pltpu.VMEM((4, 2, rows, TILE), F32),
            pltpu.VMEM((2, rows, TILE), I32),
            pltpu.VMEM((2, 2, rows, TILE), F32),
            pltpu.VMEM((2 * TILE, TILE), F32),
            pltpu.VMEM((2, TILE), F32),
            pltpu.VMEM((DEVS, 2, TILE), F32),
            pltpu.SemaphoreType.DMA((3,)),
            pltpu.SemaphoreType.DMA((2, 2, LOCAL_T)),
            pltpu.SemaphoreType.DMA((2, KT)),
            pltpu.SemaphoreType.DMA((1,)),
            pltpu.SemaphoreType.DMA((count,)),
            pltpu.SemaphoreType.DMA((count,)),
            *(pltpu.VMEM((DEVS, high - low, 8, TILE), I16) for _, low, high in CHUNKS),
            pltpu.VMEM((KT, points, TILE), BF16),
            pltpu.VMEM((KT, points, TILE), BF16),
            pltpu.VMEM((KT, points, TILE), F8),
            pltpu.VMEM((KT, points, TILE), F8),
        ],
        compiler_params=pltpu.CompilerParams(
            collective_id=0, has_side_effects=True, vmem_limit_bytes=VMEM_LIMIT
        ),
    )(first, second, basis, tile_list, tile_count, point_count, offsets, weights, atoms)


def local(
    density_first,
    density_second,
    basis,
    tile_list,
    tile_count,
    point_count,
    offsets,
    weights,
    atom_of_point,
):
    density, shared = whole(
        density_first,
        density_second,
        basis,
        tile_list,
        tile_count,
        point_count,
        offsets,
        weights,
        atom_of_point,
    )
    everyone = shared.reshape(DEVS, 2 * TILE)
    half = 4 * 18
    main = everyone[:, : 2 * half]
    extra = jnp.roll(everyone[:, 2 * half : 3 * half], 1, axis=0)
    whole_moments = main + jnp.concatenate([extra, jnp.zeros_like(extra)], axis=1)
    return (density, whole_moments.reshape(ATOMS, 18).T.reshape(2, 9, ATOMS))


def solution(mesh):
    torus = Mesh(mesh.devices.reshape(4, 4, 4, 2), ("row_0", "row_1", "col_0", "col_1"))
    in_specs = (
        P(ROW, COL),
        P(ROW, COL),
        P(ROW_COL, None, None),
        P(ROW_COL, None),
        P(ROW_COL),
        P(ROW_COL),
        P(None, ROW_COL, None),
        P(ROW_COL, None),
        P(ROW_COL, None),
    )
    out_specs = (P(None, ROW_COL, None), P())
    return jax.shard_map(local, mesh=torus, in_specs=in_specs, out_specs=out_specs, check_vma=False)
```

```python
import functools

import jax
import jax.numpy as jnp
from jax import lax
from jax.experimental import pallas as pl
from jax.experimental.pallas import tpu as pltpu
from jax.sharding import Mesh
from jax.sharding import PartitionSpec as P

TILE = 128
ATOMS = 1024
ROW = ("row_0", "row_1")
COL = ("col_0", "col_1")
ROW_COL = ("row_0", "row_1", "col_0", "col_1")
KT = 7
N_ROW = 16
N_COL = 8
DEVS = N_ROW * N_COL
NT = 96
STARTS = NT - KT + 1
LOCAL_T = NT // N_ROW
LOCAL_U = NT // N_COL
BLOCK = 2048
GROUPS = BLOCK // TILE
F32 = jnp.float32
BF16 = jnp.bfloat16
I16 = jnp.int16
I32 = jnp.int32
F8 = jnp.float8_e5m2
LOW_SCALE = 2.0**30
BASIS_SCALE = 2.0**13
LOW_UNSCALE = 2.0**-43
VMEM_LIMIT = 60 * 1024 * 1024
MESH_ID = pl.DeviceIdType.MESH
SMEM_SPEC = pl.BlockSpec(memory_space=pltpu.SMEM)
VMEM_SPEC = pl.BlockSpec(memory_space=pltpu.VMEM)
ANY_SPEC = pl.BlockSpec(memory_space=pl.ANY)


def encode(value):
    size = jnp.abs(value)
    safe = jnp.maximum(size, 2.0**-38)
    power = jnp.floor(jnp.log2(safe))
    code = (power + 37.0) * 1024.0 + safe * jnp.exp2(10.0 - power)
    code = jnp.clip(jnp.floor(code + 0.5), 0.0, 32767.0)
    code = jnp.where(size >= 2.0**-38, code, 0.0)
    code = jnp.where(value < 0.0, -code, code)
    return code.astype(I32).astype(I16)


def decode(code):
    code = code.astype(I32)
    size = jnp.abs(code)
    power = lax.shift_right_logical(size, 10).astype(F32)
    fraction = (lax.bitwise_and(size, 1023) + 1024).astype(F32)
    value = fraction * jnp.exp2(power - 48.0)
    value = jnp.where(size > 0, value, 0.0)
    return jnp.where(code < 0, -value, value)


def harmonics(x, y, z):
    radius_sq = x * x + y * y + z * z
    return [
        None,
        x,
        y,
        z,
        x * y,
        y * z,
        3.0 * z * z - radius_sq,
        x * z,
        x * x - y * y,
    ]


CHUNKS = ((0, 0, 4), (0, 4, 7), (1, 0, 4), (1, 4, 6), (1, 6, 7))
OTHERS = pl.ds(0, DEVS - 1)


def flat(spot):
    return ((spot[0] * 4 + spot[1]) * 4 + spot[2]) * 2 + spot[3]


def wait_all(ref, sem):
    pltpu.make_async_copy(ref, ref, sem).wait()


def to_everyone(spot, send):
    z, x, y, core = spot
    way = 1 - 2 * core
    zs = [(z + way * k + 4) % 4 for k in range(4)]
    xs = [(x + way * k + 4) % 4 for k in range(4)]
    first = tuple((y + way * k + 4) % 4 for k in range(4))
    both = [core, 1 - core]
    for turn in range(2):

        def step(i, ys, turn=turn):
            for n in range(16):
                b = n % 4
                a = (n // 4 + b) % 4
                partner = (zs[a], xs[b], ys[(a + b) % 4], both[(turn + a) % 2])
                if n == 0 and turn == 0:

                    @pl.when(i > 0)
                    def _(partner=partner):
                        send(partner)
                else:
                    send(partner)
            return (*ys[1:], ys[0])

        lax.fori_loop(0, 4, step, first)


def remote(source, target, send_sem, recv_sem, partner):
    pltpu.make_async_remote_copy(
        src_ref=source,
        dst_ref=target,
        send_sem=send_sem,
        recv_sem=recv_sem,
        device_id=partner,
        device_id_type=MESH_ID,
    ).start()


def extract_tile(r, e, tile, m, ul, t):
    row_tile = r + 16 * t
    if ul == 0:
        d = e
        near = 1 - e // 4
        key = row_tile + d * (1 - near)
        turned = (e >= 1) & (e <= 3)
    else:
        d = 8 - e
        near = (e + 3) // 8
        key = row_tile - d * near
        turned = e <= 4
    kind = near * d + (1 - near) * (7 - d)
    q = (kind + 4 * m + (key + 16) // 16 + 15) % 8
    value = tile.astype(F32)
    value = jnp.where(turned, value.T, value)
    return q, value.reshape(N_ROW, 8, TILE).astype(BF16)


def whole_kernel(
    first,
    second,
    basis,
    tile_list,
    tile_count,
    point_count,
    far_offsets,
    far_weights,
    far_atoms,
    density,
    moments,
    offsets,
    weights,
    atoms,
    tiles,
    banded,
    slices,
    table,
    windows,
    own_starts,
    vector_starts,
    starts,
    outgoing,
    matrix,
    low_matrix,
    kept,
    geometry,
    labels,
    dens,
    sums,
    own_moments,
    all_moments,
    point_sems,
    tile_sems,
    basis_sems,
    here_sems,
    send_sems,
    recv_sems,
    *buffers,
):
    arrived = buffers[: len(CHUNKS)]
    values = buffers[len(CHUNKS) : len(CHUNKS) + 2]
    low_values = buffers[len(CHUNKS) + 2 :]
    spot = [lax.axis_index(name) for name in ROW_COL]
    me = flat(spot)
    r = spot[0] * 4 + spot[1]
    c = spot[2] * 2 + spot[3]
    e = (c - r + 16) % 8
    points = basis.shape[1]
    rows = points // TILE
    point_copies = [
        pltpu.make_async_copy(source, target, point_sems.at[k])
        for k, (source, target) in enumerate(
            [(far_offsets, offsets), (far_weights, weights), (far_atoms, atoms)]
        )
    ]

    def tile_copy(m, ul, t):
        column = (r + 16 * t + e - 8 * ul - c + 64) // 8 - 8
        column = jnp.minimum(jnp.maximum(column, 0), LOCAL_U - 1)
        source = (first, second)[m]
        return pltpu.make_async_copy(
            source.at[pl.ds(t * TILE, TILE), pl.ds(pl.multiple_of(column * TILE, TILE), TILE)],
            tiles.at[m, ul, t],
            tile_sems.at[m, ul, t],
        )

    def basis_copy(b, j):
        return pltpu.make_async_copy(
            basis.at[b, :, pl.ds(j * TILE, TILE)], values[b].at[j], basis_sems.at[b, j]
        )

    todo = [(m, ul, t) for m in range(2) for ul in range(2) for t in range(LOCAL_T)]
    for item in todo:
        tile_copy(*item).start()
    for copy in point_copies:
        copy.start()
    barrier = pltpu.get_barrier_semaphore()
    to_everyone(
        spot,
        lambda partner: pl.semaphore_signal(
            barrier, inc=1, device_id=partner, device_id_type=MESH_ID
        ),
    )

    listed = [[tile_list[b, p] for p in range(KT)] for b in range(2)]
    begin = [functools.reduce(jnp.minimum, one) for one in listed]
    place = [
        [
            jnp.minimum(
                sum(jnp.where(listed[b][p] == begin[b] + t, p, 0) for p in range(KT)), KT - 1
            )
            for t in range(KT)
        ]
        for b in range(2)
    ]
    live = [[(place[b][t] < tile_count[b]).astype(F32) for t in range(KT)] for b in range(2)]
    lane = lax.broadcasted_iota(I32, (1, TILE), 1)
    own_starts[...] = jnp.where(lane == 0, begin[0], begin[1])

    banded[...] = jnp.zeros(banded.shape, BF16)
    for m, ul, t in todo:
        tile_copy(m, ul, t).wait()
        q, value = extract_tile(r, e, tiles[m, ul, t], m, ul, t)
        banded[:, q, ul, m] = value
    pl.semaphore_wait(barrier, DEVS - 1)

    for ul in range(2):

        @pl.when((e <= 6) if ul == 0 else (e >= 2))
        def _(ul=ul):
            to_everyone(
                spot,
                lambda to: remote(
                    banded.at[to[0] * 4 + to[1], to[2] * 2 + to[3], ul],
                    slices.at[me, ul],
                    send_sems.at[1 + ul],
                    recv_sems.at[1 + ul],
                    to,
                ),
            )

    to_everyone(
        spot,
        lambda to: remote(
            own_starts, vector_starts.at[me], send_sems.at[0], recv_sems.at[0], to
        ),
    )
    vector_starts[me] = own_starts[...]
    slices[me] = banded[r, c]
    for b in range(2):
        for j in range(KT):
            basis_copy(b, j).start()
    for copy in point_copies:
        copy.wait()
    for b in range(2):
        for i in range(rows):
            lanes = pl.ds(i * TILE, TILE)
            for k in range(3):
                geometry[k, b, pl.ds(i, 1), :] = offsets[k, pl.ds(b, 1), lanes]
            geometry[3, b, pl.ds(i, 1), :] = weights[pl.ds(b, 1), lanes]
            labels[b, pl.ds(i, 1), :] = atoms[pl.ds(b, 1), lanes]
    wait_all(vector_starts.at[OTHERS], recv_sems.at[0])
    scalars = pltpu.make_async_copy(vector_starts, starts, here_sems.at[0])
    scalars.start()
    scalars.wait()
    for ul in range(2):
        senders = (112, 96)[ul]
        takes_part = (e <= 6) if ul == 0 else (e >= 2)

        @pl.when(takes_part)
        def _(ul=ul, senders=senders):
            wait_all(slices.at[pl.ds(0, senders - 1), ul], recv_sems.at[1 + ul])

        @pl.when(jnp.logical_not(takes_part))
        def _(ul=ul, senders=senders):
            wait_all(slices.at[pl.ds(0, senders), ul], recv_sems.at[1 + ul])

    def kind_of(k):
        return lax.bitwise_and(c - lax.shift_right_logical(k, 4), 7)

    def owner(row_tile, col_tile):
        return lax.bitwise_and(row_tile, 15) * 8 + lax.bitwise_and(col_tile, 7)

    def fill(k, carry):
        which = kind_of(k)
        kind = lax.bitwise_and(which, 3)
        m = lax.shift_right_logical(which, 2)
        far = k + kind
        paired = lax.shift_right_logical(kind + 3, 2)
        upper = slices[owner(k, far), 0, m].astype(F32)
        lower = slices[owner(far, k), paired, m].astype(F32)
        table[2 * k] = encode(upper + lower * paired.astype(F32))
        near = k + 9 + kind + (1 - paired)
        upper = slices[owner(near, k), 0, m].astype(F32)
        lower = slices[owner(k, near + 8), 1, m].astype(F32)
        table[2 * k + 1] = encode(upper + lower)
        return carry

    lax.fori_loop(0, NT, fill, 0, unroll=8)

    def window(a, carry):
        for t in range(KT):
            kind = lax.bitwise_and(kind_of(a + t), 3)
            wraps = lax.shift_right_logical(t + kind + 1, 3)
            windows[a, t] = table[2 * (a + t) + wraps]
        return carry

    lax.fori_loop(0, STARTS, window, 0, unroll=5)

    for b in range(2):

        def pack(d, carry, b=b):
            outgoing[b, d] = windows[starts[d, 0, b]]
            return carry

        lax.fori_loop(0, DEVS, pack, 0, unroll=8)

    for n, (b, low, high) in enumerate(CHUNKS):
        part = pl.ds(low, high - low)
        to_everyone(
            spot,
            lambda to, n=n, b=b, part=part: remote(
                outgoing.at[b, flat(to), part],
                arrived[n].at[me],
                send_sems.at[3 + n],
                recv_sems.at[3 + n],
                to,
            ),
        )
        arrived[n][me] = outgoing[b, me, part]

    spots = lax.broadcasted_iota(I32, (rows, TILE), 0) * TILE + lax.broadcasted_iota(
        I32, (rows, TILE), 1
    )
    for n, (b, low, high) in enumerate(CHUNKS):
        begins = low == 0
        ends = high == KT
        if n == 0:
            for each in range(2):
                for j in range(KT):
                    basis_copy(each, j).wait()

                    def narrow(i, carry, each=each, j=j):
                        span = pl.ds(pl.multiple_of(i * BLOCK, BLOCK), BLOCK)
                        value = values[each][j, span, :].astype(F32) * BASIS_SCALE
                        low_values[each][j, span, :] = value.astype(F8)
                        return carry

                    lax.fori_loop(0, points // BLOCK, narrow, 0)
        wait_all(arrived[n].at[OTHERS], recv_sems.at[3 + n])
        for t in range(low, high):
            turn = lax.shift_right_arithmetic(begin[b] + t, 4)
            for kind in range(4):
                alive = live[b][t] * live[b][(t + kind) % KT]
                for m in range(2):
                    q = lax.bitwise_and(kind + 4 * m + turn, 7)
                    codes = [arrived[n][s * N_COL + q, t - low] for s in range(N_ROW)]
                    value = decode(jnp.concatenate(codes, axis=0)) * alive
                    upper = value.astype(BF16)
                    lower = (value - upper.astype(F32)) * LOW_SCALE
                    columns = pl.ds(m * TILE, TILE)
                    matrix[t, pl.ds(kind * TILE, TILE), columns] = upper
                    low_matrix[t, pl.ds(kind * TILE, TILE), columns] = lower.astype(F8)

        def step(block, carry, b=b, low=low, high=high, begins=begins, ends=ends):
            span = pl.ds(pl.multiple_of(block * BLOCK, BLOCK), BLOCK)
            total = None if begins else kept[span, :]
            for t in range(low, high):
                order = [place[b][(t + i) % KT] for i in range(4)]
                left = jnp.concatenate([values[b][p, span, :] for p in order], axis=1)
                low_left = jnp.concatenate([low_values[b][p, span, :] for p in order], axis=1)
                product = jnp.dot(left, matrix[t], preferred_element_type=F32)
                low = jnp.dot(low_left, low_matrix[t], preferred_element_type=F32)
                product = product + low * LOW_UNSCALE
                own = left[:, :TILE].astype(F32)
                term = product * jnp.concatenate([own, own], axis=1)
                total = term if total is None else total + term
            if not ends:
                kept[span, :] = total
            else:
                for m in range(2):
                    for i in range(GROUPS):
                        part = total[i * TILE : (i + 1) * TILE, m * TILE : (m + 1) * TILE]
                        dens[m, b, pl.ds(block * GROUPS + i, 1), :] = jnp.sum(
                            part.T, axis=0, keepdims=True
                        )
            return carry

        lax.fori_loop(0, points // BLOCK, step, 0)
        if not ends:
            continue
        inside = spots < point_count[b]
        harmonic = harmonics(geometry[0, b], geometry[1, b], geometry[2, b])
        weight = geometry[3, b]
        factors = [weight] + [weight * item for item in harmonic[1:]]
        base = (me * 8 + b * 4) % ATOMS
        hits = [labels[b] == (base + j) % ATOMS for j in range(8)]
        if b == 0:
            sums[...] = jnp.zeros(sums.shape, F32)
        for m in range(2):
            value = jnp.where(inside, dens[m, b], 0.0)
            dens[m, b] = value
            for h in range(9):
                term = value * factors[h]
                for j in range(8):
                    line = jnp.sum(jnp.where(hits[j], term, 0.0), axis=0, keepdims=True)
                    at = pl.ds((j + 4 * b) * 18 + m * 9 + h, 1)
                    sums[at, :] = line if b == 0 or j >= 4 else sums[at, :] + line
    for i in range(2):
        part = sums[pl.ds(i * TILE, TILE), :]
        own_moments[pl.ds(i, 1), :] = jnp.sum(part.T, axis=0, keepdims=True)
    for m in range(2):
        for b in range(2):
            for i in range(rows):
                density[m, pl.ds(b, 1), pl.ds(i * TILE, TILE)] = dens[m, b, pl.ds(i, 1), :]
    last = 3 + len(CHUNKS)
    to_everyone(
        spot,
        lambda to: remote(
            own_moments, all_moments.at[me], send_sems.at[last], recv_sems.at[last], to
        ),
    )
    all_moments[me] = own_moments[...]
    wait_all(vector_starts.at[OTHERS], send_sems.at[0])
    for ul in range(2):

        @pl.when((e <= 6) if ul == 0 else (e >= 2))
        def _(ul=ul):
            wait_all(slices.at[OTHERS, ul], send_sems.at[1 + ul])

    for n in range(len(CHUNKS)):
        wait_all(arrived[n].at[OTHERS], send_sems.at[3 + n])
    wait_all(all_moments.at[OTHERS], send_sems.at[last])
    wait_all(all_moments.at[OTHERS], recv_sems.at[last])
    moments[...] = all_moments[...]


def whole(first, second, basis, tile_list, tile_count, point_count, offsets, weights, atoms):
    points = basis.shape[1]
    rows = points // TILE
    count = 4 + len(CHUNKS)
    return pl.pallas_call(
        whole_kernel,
        name="whole",
        out_shape=(
            jax.ShapeDtypeStruct((2, 2, points), F32),
            jax.ShapeDtypeStruct((DEVS, 2, TILE), F32),
        ),
        in_specs=[ANY_SPEC] * 3 + [SMEM_SPEC] * 3 + [ANY_SPEC] * 3,
        out_specs=(VMEM_SPEC, VMEM_SPEC),
        scratch_shapes=[
            pltpu.VMEM(offsets.shape, F32),
            pltpu.VMEM(weights.shape, F32),
            pltpu.VMEM(atoms.shape, I32),
            pltpu.VMEM((2, 2, LOCAL_T, TILE, TILE), BF16),
            pltpu.VMEM((N_ROW, N_COL, 2, 2, 8, TILE), BF16),
            pltpu.VMEM((DEVS, 2, 2, 8, TILE), BF16),
            pltpu.VMEM((2 * NT, 8, TILE), I16),
            pltpu.VMEM((STARTS, KT, 8, TILE), I16),
            pltpu.VMEM((1, TILE), I32),
            pltpu.VMEM((DEVS, 1, TILE), I32),
            pltpu.SMEM((DEVS, 1, TILE), I32),
            pltpu.VMEM((2, DEVS, KT, 8, TILE), I16),
            pltpu.VMEM((KT, 4 * TILE, 2 * TILE), BF16),
            pltpu.VMEM((KT, 4 * TILE, 2 * TILE), F8),
            pltpu.VMEM((points, 2 * TILE), F32),
            pltpu.VMEM((4, 2, rows, TILE), F32),
            pltpu.VMEM((2, rows, TILE), I32),
            pltpu.VMEM((2, 2, rows, TILE), F32),
            pltpu.VMEM((2 * TILE, TILE), F32),
            pltpu.VMEM((2, TILE), F32),
            pltpu.VMEM((DEVS, 2, TILE), F32),
            pltpu.SemaphoreType.DMA((3,)),
            pltpu.SemaphoreType.DMA((2, 2, LOCAL_T)),
            pltpu.SemaphoreType.DMA((2, KT)),
            pltpu.SemaphoreType.DMA((1,)),
            pltpu.SemaphoreType.DMA((count,)),
            pltpu.SemaphoreType.DMA((count,)),
            *(pltpu.VMEM((DEVS, high - low, 8, TILE), I16) for _, low, high in CHUNKS),
            pltpu.VMEM((KT, points, TILE), BF16),
            pltpu.VMEM((KT, points, TILE), BF16),
            pltpu.VMEM((KT, points, TILE), F8),
            pltpu.VMEM((KT, points, TILE), F8),
        ],
        compiler_params=pltpu.CompilerParams(
            collective_id=0, has_side_effects=True, vmem_limit_bytes=VMEM_LIMIT
        ),
    )(first, second, basis, tile_list, tile_count, point_count, offsets, weights, atoms)


def local(
    density_first,
    density_second,
    basis,
    tile_list,
    tile_count,
    point_count,
    offsets,
    weights,
    atom_of_point,
):
    density, shared = whole(
        density_first,
        density_second,
        basis,
        tile_list,
        tile_count,
        point_count,
        offsets,
        weights,
        atom_of_point,
    )
    everyone = shared.reshape(DEVS, 2 * TILE)
    half = 4 * 18
    main = everyone[:, : 2 * half]
    extra = jnp.roll(everyone[:, 2 * half : 3 * half], 1, axis=0)
    whole_moments = main + jnp.concatenate([extra, jnp.zeros_like(extra)], axis=1)
    return (density, whole_moments.reshape(ATOMS, 18).T.reshape(2, 9, ATOMS))


def solution(mesh):
    torus = Mesh(mesh.devices.reshape(4, 4, 4, 2), ("row_0", "row_1", "col_0", "col_1"))
    in_specs = (
        P(ROW, COL),
        P(ROW, COL),
        P(ROW_COL, None, None),
        P(ROW_COL, None),
        P(ROW_COL),
        P(ROW_COL),
        P(None, ROW_COL, None),
        P(ROW_COL, None),
        P(ROW_COL, None),
    )
    out_specs = (P(None, ROW_COL, None), P())
    return jax.shard_map(local, mesh=torus, in_specs=in_specs, out_specs=out_specs, check_vma=False)
```
